1024 devices in a mesh: dp: 32 (over x, z_lo), fsdp: 8 (over z_hi, core), tp: 4 (over y).
Axes of the slice: x: 4, y: 4, z: 32 (z_hi: 4, z_lo: 8; z = z_hi * 8 + z_lo), core: 2. Of those that a mesh axis runs over, the one named last changes fastest.
Arguments:
- hidden: bfloat16 [131072, 7168], P(('dp', 'fsdp')), may hold values from -6 to 6
- cotangent: bfloat16 [131072, 576], P(('dp', 'fsdp'), 'tp'), may hold values from -6 to 6
- rewards: int32 [1024], P(('dp', 'fsdp')), may hold values from 0 to 8
- groups: int32 [1024], P(('dp', 'fsdp')), may hold values from 0 to 63, as said below
- lengths: int32 [1024], P(('dp', 'fsdp')), may hold values from 1 to 128
- master: float32 [8, 896, 576], P('fsdp', 'dp', 'tp'), may hold values from -6 to 6
Outputs:
- grad_owned: float32 [8, 896, 576], P('fsdp', 'dp', 'tp')
- rollout: bfloat16 [8, 896, 576], P('fsdp')
The draws below stay inside these ranges and needn't reach their ends.
Inputs may be any that keep to these rules, and one draw needn't show every extreme that they name: `groups`: each prompt number names exactly 16 samples.
All inputs are finite; a program needn't handle non-finite values.
Results may differ from the reference program's by a relative error of at most 0.0033.
Values may be sent and summed in bfloat16 or wider, within the bound.
No kernel may reach another device: no remote copies, remote signals or barrier semaphores. Data moves between devices by JAX's collectives and lax.ppermute only.
A program may use at most 64 MiB of HBM per device.

```python
import jax
import jax.numpy as jnp
from jax import lax

D = 7168
R = 576
GROUP = 16
SEQ = 128
TOK_DEV = 512
SAMPLES = 1024
TOKENS = 131072
GROUPS = 64
N_FSDP = 8


def draw_groups(key, part):
    order = jax.random.permutation(jax.random.fold_in(key, 7), SAMPLES)
    return (order // GROUP).astype(jnp.int32)


def plant(entries, stream_key, least, high):
    shape = entries.shape
    index_at = [jax.random.randint(jax.random.fold_in(stream_key, axis), (), 0, shape[axis]) for axis in range(len(shape))]
    entries = entries.at[tuple(index_at)].set(least)
    longest = shape.index(max(shape))
    index_at[longest] = (index_at[longest] + 1) % shape[longest]
    return entries.at[tuple(index_at)].set(high)


def levels(own_key, shape, split, low, largest):
    def one(axis_at, parts):
        steps = jax.random.uniform(jax.random.fold_in(jax.random.fold_in(own_key, 6), axis_at), (parts,), jnp.float32, low / len(split), largest / len(split))
        return jnp.repeat(jnp.exp(steps), shape[axis_at] // parts).reshape((-1,) + (1,) * (len(shape) - axis_at - 1))

    loudness = one(*split[0])
    for cut in split[1:]:
        loudness = loudness * one(*cut)
    return loudness


def scatter_about(own_key, extent, scale, bound, shards=(), kind=jnp.bfloat16):
    result = scale * jax.random.normal(own_key, extent, jnp.float32)
    if shards:
        result = result * levels(own_key, extent, shards, -0.22, 0.18)
    return jnp.clip(result, -bound, bound).astype(kind)


def setup_inputs(seed: int = 0) -> dict:
    splits = jax.random.split(jax.random.key(seed), 7)
    return {
        "hidden": scatter_about(splits[0], (TOKENS, D), 1.0, 6.0, ((0, 256),)),
        "cotangent": scatter_about(splits[1], (TOKENS, R), 1.0, 6.0, ((0, 256), (1, 4))),
        "rewards": plant(jax.random.randint(splits[2], (SAMPLES,), 0, 9), jax.random.fold_in(splits[2], 1), 0, 8).astype(jnp.int32),
        "groups": draw_groups(jax.random.fold_in(splits[6], 71), 0),
        "lengths": plant(jax.random.randint(splits[4], (SAMPLES,), 1, SEQ + 1), jax.random.fold_in(splits[4], 1), 1, SEQ).astype(jnp.int32),
        "master": scatter_about(splits[5], (N_FSDP, D // N_FSDP, R), 1.0, 6.0, ((0, 8), (1, 32), (2, 4)), jnp.float32),
    }


def reference(hidden, cotangent, rewards, groups, lengths, master):
    labels = jnp.arange(GROUPS, dtype=jnp.int32)
    onehot = (groups[:, None] == labels[None, :]).astype(jnp.float32)
    reward_f = rewards.astype(jnp.float32)
    totals = jnp.dot(reward_f, onehot, precision=lax.Precision.HIGHEST)
    squares = jnp.dot(reward_f * reward_f, onehot, precision=lax.Precision.HIGHEST)
    group_mean = totals / GROUP
    group_square = squares / GROUP
    sample_mean = jnp.dot(onehot, group_mean, precision=lax.Precision.HIGHEST)
    sample_square = jnp.dot(onehot, group_square, precision=lax.Precision.HIGHEST)
    advantage = (reward_f - sample_mean) / jnp.sqrt(sample_square - sample_mean * sample_mean + 1.0)
    positions = jnp.arange(SEQ, dtype=jnp.int32)
    live = (positions[None, :] < lengths[:, None]).astype(jnp.float32)
    scale = (advantage[:, None] * live / lengths[:, None].astype(jnp.float32)).reshape(TOKENS)
    weighted = (cotangent.astype(jnp.float32) * scale[:, None]).astype(jnp.bfloat16)
    blocks = TOKENS // TOK_DEV
    hidden_blocks = hidden.reshape(blocks, TOK_DEV, D)
    weighted_blocks = weighted.reshape(blocks, TOK_DEV, R)

    def add_block(carry, pair):
        left = pair[0].astype(jnp.float32)
        right = pair[1].astype(jnp.float32)
        return (carry + jnp.dot(left.T, right, precision=lax.Precision.HIGHEST), None)
    grad, _ = lax.scan(add_block, jnp.zeros((D, R), jnp.float32), (hidden_blocks, weighted_blocks))
    grad_owned = grad.reshape(N_FSDP, D // N_FSDP, R)
    rollout = (master - 0.1 * grad_owned).astype(jnp.bfloat16)
    return (grad_owned, rollout)
```

```python
import jax
import jax.numpy as jnp
from jax import lax
from jax.experimental import pallas as pl
from jax.experimental.pallas import tpu as pltpu
from jax.sharding import Mesh
from jax.sharding import PartitionSpec as P

GROUP = 16
X, ZL, ZH, CORE, TP = "x", "z_lo", "z_hi", "core", "tp"
DP = (X, ZL)
FSDP = (ZH, CORE)
DP_FSDP = (X, ZL, ZH, CORE)

ROWS = 896
COLS = 144
OWN = 28
QROW = 40
LANE = 128
f32 = jnp.float32
bf16 = jnp.bfloat16


def lane_iota(rows):
    return lax.broadcasted_iota(jnp.int32, (rows, LANE), 1)


def roll(tile, shift):
    shift = shift % LANE
    return tile if shift == 0 else pltpu.roll(tile, shift, 1)


def put(acc, tiles, src, dst, width):
    lane = lane_iota(acc.shape[0])
    done = 0
    while done < width:
        tile, off = divmod(src + done, LANE)
        take = min(LANE - off, width - done)
        at = dst + done
        moved = roll(tiles(tile), at - off)
        acc = jnp.where((lane >= at) & (lane < at + take), moved, acc)
        done += take
    return acc


def grad_body(scal, seen, own_c, oth_c, own_h, oth_h, out, w_own, w_oth, prod):
    step = pl.program_id(0)

    @pl.when(step == 0)
    def _():
        seen_r = seen[:, 0:32].astype(f32)
        seen_g = seen[:, 32:64]
        pos = lax.broadcasted_iota(jnp.int32, (1, LANE), 1)
        for s in range(8):
            hit = seen_g == scal[9 + s]
            total = jnp.sum(jnp.where(hit, seen_r, 0.0), axis=(0, 1), keepdims=True)
            square = jnp.sum(jnp.where(hit, seen_r * seen_r, 0.0), axis=(0, 1), keepdims=True)
            mean = total / GROUP
            var = square / GROUP - mean * mean
            reward = jnp.full((1, 1), scal[1 + s], jnp.int32).astype(f32)
            adv = (reward - mean) / jnp.sqrt(var + 1.0)
            size = jnp.full((1, 1), scal[17 + s], jnp.int32).astype(f32)
            live = jnp.where(pos < scal[17 + s], 1.0, 0.0)
            scale = adv * live / size
            src, dst = (own_c, w_own) if s < 4 else (oth_c, w_oth)
            at = (s % 4) * LANE
            dst[:, at : at + LANE] = (src[:, at : at + LANE].astype(f32) * scale).astype(bf16)

    block = jnp.dot(w_own[...], own_h[...], preferred_element_type=f32)
    block += jnp.dot(w_oth[...], oth_h[...], preferred_element_type=f32)
    prod[step] = block

    @pl.when(step == pl.num_programs(0) - 1)
    def _():
        for x in range(4):
            for t in range(ROWS // LANE):
                acc = jnp.zeros((COLS, LANE), f32)
                for j in range(4):
                    lo = max(j * 224, t * LANE)
                    hi = min(j * 224 + 224, t * LANE + LANE)
                    if lo < hi:
                        at = x * 224 + lo - j * 224
                        tiles = lambda k, j=j: prod[j, :, k * LANE : (k + 1) * LANE]
                        acc = put(acc, tiles, at, lo - t * LANE, hi - lo)
                out[x, :, t * LANE : (t + 1) * LANE] = acc.astype(bf16)


def grad_parts(scal, seen, own_c, oth_c, own_h, oth_h):
    tokens = own_h.shape[0]
    half = pl.BlockSpec((tokens, ROWS), lambda j, scal: (0, 2 * j + scal[0]))
    whole = lambda shape: pl.BlockSpec(shape, lambda j, scal: (0,) * len(shape))
    return pl.pallas_call(
        grad_body,
        out_shape=jax.ShapeDtypeStruct((4, COLS, ROWS), bf16),
        grid_spec=pltpu.PrefetchScalarGridSpec(
            num_scalar_prefetch=1,
            grid=(4,),
            in_specs=[
                whole(seen.shape),
                whole(own_c.shape),
                whole(oth_c.shape),
                half,
                half,
            ],
            out_specs=whole((4, COLS, ROWS)),
            scratch_shapes=[
                pltpu.VMEM((COLS, tokens), bf16),
                pltpu.VMEM((COLS, tokens), bf16),
                pltpu.VMEM((4, COLS, ROWS), f32),
            ],
        ),
        compiler_params=pltpu.CompilerParams(dimension_semantics=("arbitrary",)),
        name="grad_parts",
    )(scal, seen, own_c, oth_c, own_h, oth_h)


def x_body(parts, out, total):
    for t in range(ROWS // LANE):
        at = slice(t * LANE, (t + 1) * LANE)
        total[t] = (parts[0, :, at].astype(f32) + parts[1, :, at].astype(f32)) + (
            parts[2, :, at].astype(f32) + parts[3, :, at].astype(f32)
        )
    for z in range(8):
        acc = jnp.zeros((COLS, LANE), f32)
        for j in range(4):
            acc = put(acc, lambda k: total[k], j * 224 + z * OWN, j * 32, OWN)
        out[z] = acc.astype(bf16)


def x_sum(parts):
    return pl.pallas_call(
        x_body,
        out_shape=jax.ShapeDtypeStruct((8, COLS, LANE), bf16),
        scratch_shapes=[pltpu.VMEM((ROWS // LANE, COLS, LANE), f32)],
        name="x_sum",
    )(parts)


def zl_body(parts, out, total):
    acc = parts[0].astype(f32)
    for z in range(1, 8):
        acc += parts[z].astype(f32)
    total[0:COLS] = acc
    total[COLS:] = jnp.zeros((4 * QROW - COLS, LANE), f32)
    for j in range(4):
        acc = jnp.zeros((QROW, LANE), f32)
        for q in range(4):
            rows = total[q * QROW : (q + 1) * QROW]
            acc = put(acc, lambda k: rows, j * 32, q * 32, 32)
        out[j] = acc.astype(bf16)


def zl_sum(parts):
    return pl.pallas_call(
        zl_body,
        out_shape=jax.ShapeDtypeStruct((4, QROW, LANE), bf16),
        scratch_shapes=[pltpu.VMEM((4 * QROW, LANE), f32)],
        name="zl_sum",
    )(parts)


def zh_body(parts, master, grad, copies):
    total = (parts[0].astype(f32) + parts[1].astype(f32)) + (
        parts[2].astype(f32) + parts[3].astype(f32)
    )
    grad[...] = total
    new = (master[...] - 0.1 * total).astype(bf16)
    for z in range(8):
        copies[z] = new


def zh_sum(parts, master):
    return pl.pallas_call(
        zh_body,
        out_shape=(
            jax.ShapeDtypeStruct((QROW, LANE), f32),
            jax.ShapeDtypeStruct((8, QROW, LANE), bf16),
        ),
        name="zh_sum",
    )(parts, master)


def rows_body(parts, out, wide):
    for x in range(4):
        for z in range(8):
            wide[x * 8 + z] = parts[x, z].astype(f32)
    for t in range(ROWS // LANE):
        for q in range(4):
            acc = jnp.zeros((QROW, LANE), f32)
            for d in range(32):
                lo = max(d * OWN, t * LANE)
                hi = min(d * OWN + OWN, t * LANE + LANE)
                if lo < hi:
                    acc = put(acc, lambda k: wide[d], q * 32 + lo - d * OWN, lo - t * LANE, hi - lo)
            rows = min(QROW, COLS - q * QROW)
            out[q * QROW : q * QROW + rows, t * LANE : (t + 1) * LANE] = acc[:rows].astype(bf16)


def row_block(parts):
    return pl.pallas_call(
        rows_body,
        out_shape=jax.ShapeDtypeStruct((COLS, ROWS), bf16),
        scratch_shapes=[pltpu.VMEM((32, QROW, LANE), f32)],
        name="row_block",
    )(parts)


def pack(master):
    wide = jnp.pad(master.T, ((0, 4 * QROW - COLS), (0, 32 - OWN)))
    return wide.reshape(4, QROW, 32).transpose(1, 0, 2).reshape(QROW, LANE)


def unpack(grad):
    wide = grad.reshape(QROW, 4, 32).transpose(1, 0, 2).reshape(4 * QROW, 32)
    return wide[:COLS, :OWN].T


def exchange(array, axis):
    return lax.all_to_all(array, axis, split_axis=0, concat_axis=0, tiled=True)


def shards(hidden, cotangent, rewards, groups, lengths, master):
    swap = [(0, 1), (1, 0)]
    other_hidden = lax.ppermute(hidden, CORE, swap)
    cot = cotangent.T
    other_cot = lax.ppermute(cot, CORE, swap)
    mine = jnp.stack([rewards, groups, lengths])
    chip = lax.all_gather(mine, CORE)
    other = chip[0] + chip[1] - mine
    plane = lax.all_gather(chip[:, :2], X)
    line = plane.transpose(2, 0, 1, 3).reshape(64)
    copies = jnp.broadcast_to(jnp.pad(line, (0, 64)), (32, LANE))
    seen = exchange(copies, (ZH, ZL))
    core = lax.axis_index(CORE).astype(jnp.int32)
    scal = jnp.concatenate([core[None], jnp.stack([mine, other], axis=1).reshape(24)])
    parts = grad_parts(scal, seen, cot, other_cot, hidden, other_hidden)
    parts = x_sum(exchange(parts, X))
    parts = zl_sum(exchange(parts, ZL))
    grad, copies = zh_sum(exchange(parts, ZH), pack(master[0]))
    line = exchange(copies, ZL)
    plane = lax.all_gather(line, X)
    block = row_block(plane)
    rollout = lax.all_gather(block, TP)
    rollout = rollout.reshape(4 * COLS, ROWS).T
    return (unpack(grad)[None], rollout[None])


def solution(mesh):
    torus = Mesh(
        mesh.devices.reshape(4, 8, 4, 2, mesh.shape["tp"]),
        (X, ZL, ZH, CORE, TP),
    )
    placed = (
        P(DP_FSDP, None),
        P(DP_FSDP, TP),
        P(DP_FSDP),
        P(DP_FSDP),
        P(DP_FSDP),
        P(FSDP, DP, TP),
    )
    return jax.shard_map(
        shards,
        mesh=torus,
        in_specs=placed,
        out_specs=(P(FSDP, DP, TP), P(FSDP, None, None)),
        check_vma=False,
    )
```

```python
import jax
import jax.numpy as jnp
from jax import lax
from jax.experimental import pallas as pl
from jax.experimental.pallas import tpu as pltpu
from jax.sharding import Mesh
from jax.sharding import PartitionSpec as P


GROUP = 16
X, ZL, ZH, CORE, TP = "x", "z_lo", "z_hi", "core", "tp"
DP = (X, ZL)
FSDP = (ZH, CORE)
DP_FSDP = (X, ZL, ZH, CORE)

ROWS = 896
COLS = 144
OWN = 28
PART = 224
STRIPE = 32
REST = 16
LANE = 128
IN_VMEM = pl.BlockSpec(memory_space=pltpu.VMEM)
f32 = jnp.float32
bf16 = jnp.bfloat16


def lane_iota(rows):
    return lax.broadcasted_iota(jnp.int32, (rows, LANE), 1)


def roll(tile, shift):
    shift = shift % LANE
    return tile if shift == 0 else pltpu.roll(tile, shift, 1)


def put(acc, tiles, src, dst, width):
    lane = lane_iota(acc.shape[0])
    done = 0
    while done < width:
        tile, off = divmod(src + done, LANE)
        take = min(LANE - off, width - done)
        at = dst + done
        moved = roll(tiles(tile), at - off)
        acc = jnp.where((lane >= at) & (lane < at + take), moved, acc)
        done += take
    return acc


def grad_body(scal, seen, own_c, oth_c, own_h, oth_h, out, w_own, w_oth, edge):
    step = pl.program_id(0)

    @pl.when(step == 0)
    def _():
        seen_r = seen[:, 0:32].astype(f32)
        seen_g = seen[:, 32:64]
        pos = lax.broadcasted_iota(jnp.int32, (1, LANE), 1)
        for s in range(8):
            hit = seen_g == scal[9 + s]
            total = jnp.sum(jnp.where(hit, seen_r, 0.0), axis=(0, 1), keepdims=True)
            square = jnp.sum(jnp.where(hit, seen_r * seen_r, 0.0), axis=(0, 1), keepdims=True)
            mean = total / GROUP
            var = square / GROUP - mean * mean
            reward = jnp.full((1, 1), scal[1 + s], jnp.int32).astype(f32)
            adv = (reward - mean) / jnp.sqrt(var + 1.0)
            size = jnp.full((1, 1), scal[17 + s], jnp.int32).astype(f32)
            live = jnp.where(pos < scal[17 + s], 1.0, 0.0)
            scale = adv * live / size
            src, dst = (own_c, w_own) if s < 4 else (oth_c, w_oth)
            at = (s % 4) * LANE
            dst[:, at : at + LANE] = (src[:, at : at + LANE].astype(f32) * scale).astype(bf16)

    block = jnp.dot(w_own[...], own_h[...], preferred_element_type=f32)
    block += jnp.dot(w_oth[...], oth_h[...], preferred_element_type=f32)

    def place(j):
        lo, hi = j * PART, (j + 1) * PART
        tiles = lambda k: block[:, k * LANE : (k + 1) * LANE]
        for x in range(4):
            for t in range(lo // LANE, -(-hi // LANE)):
                begin, end = max(lo, t * LANE), min(hi, (t + 1) * LANE)
                acc = edge[x] if t * LANE < lo else jnp.zeros((COLS, LANE), f32)
                acc = put(acc, tiles, x * PART + begin - lo, begin - t * LANE, end - begin)
                if end == (t + 1) * LANE:
                    out[x, :, t * LANE : end] = acc.astype(bf16)
                else:
                    edge[x] = acc

    for j in range(4):
        pl.when(step == j)(lambda j=j: place(j))


def grad_parts(scal, seen, own_c, oth_c, own_h, oth_h):
    tokens = own_h.shape[0]
    half = pl.BlockSpec((tokens, ROWS), lambda j, scal: (0, 2 * j + scal[0]))
    whole = lambda shape: pl.BlockSpec(shape, lambda j, scal: (0,) * len(shape))
    return pl.pallas_call(
        grad_body,
        out_shape=pltpu.VMEM((4, COLS, ROWS), bf16),
        grid_spec=pltpu.PrefetchScalarGridSpec(
            num_scalar_prefetch=1,
            grid=(4,),
            in_specs=[
                IN_VMEM,
                IN_VMEM,
                IN_VMEM,
                half,
                half,
            ],
            out_specs=whole((4, COLS, ROWS)),
            scratch_shapes=[
                pltpu.VMEM((COLS, tokens), bf16),
                pltpu.VMEM((COLS, tokens), bf16),
                pltpu.VMEM((4, COLS, LANE), f32),
            ],
        ),
        compiler_params=pltpu.CompilerParams(dimension_semantics=("arbitrary",)),
        name="grad_parts",
    )(scal, in_vmem(seen), in_vmem(own_c), in_vmem(oth_c), own_h, oth_h)


def x_body(parts, out, total, rest):
    for t in range(ROWS // LANE):
        at = slice(t * LANE, (t + 1) * LANE)
        tile = (parts[0, :, at].astype(f32) + parts[1, :, at].astype(f32)) + (
            parts[2, :, at].astype(f32) + parts[3, :, at].astype(f32)
        )
        total[t] = tile
        rest[at, 0:REST] = tile[4 * STRIPE :, :].T
    rest[ROWS:, 0:REST] = jnp.zeros((8, REST), f32)
    lane = lane_iota(STRIPE)
    for j in range(4):
        for z in range(8):
            at = j * PART + z * OWN
            last = roll(rest[at : at + STRIPE], 4 * OWN)
            acc = jnp.where(lane >= 4 * OWN, last, 0.0)
            for q in range(4):
                acc = put(acc, lambda k: total[k, q * STRIPE : (q + 1) * STRIPE], at, q * OWN, OWN)
            out[j * 8 + z] = acc.astype(bf16)


def x_sum(parts):
    return pl.pallas_call(
        x_body,
        out_shape=pltpu.VMEM((32, STRIPE, LANE), bf16),
        in_specs=[IN_VMEM],
        out_specs=IN_VMEM,
        scratch_shapes=[
            pltpu.VMEM((ROWS // LANE, COLS, LANE), f32),
            pltpu.VMEM((ROWS + 8, LANE), f32),
        ],
        name="x_sum",
    )(in_vmem(parts))


def z_body(parts, master, grad, copies):
    sums = [parts[z].astype(f32) for z in range(32)]
    while len(sums) > 1:
        sums = [a + b for a, b in zip(sums[::2], sums[1::2])]
    grad[...] = sums[0]
    new = (master[...] - 0.1 * sums[0]).astype(bf16)
    for d in range(32):
        copies[d] = new


def z_sum(parts, master):
    return pl.pallas_call(
        z_body,
        out_shape=(
            pltpu.VMEM((STRIPE, LANE), f32),
            pltpu.VMEM((32, STRIPE, LANE), bf16),
        ),
        in_specs=[IN_VMEM, IN_VMEM],
        out_specs=(IN_VMEM, IN_VMEM),
        name="z_sum",
    )(in_vmem(parts), in_vmem(master))


def rows_body(parts, out, wide, rest):
    for d in range(32):
        piece = parts[d].astype(f32)
        wide[d] = piece
        rest[d * OWN : (d + 1) * OWN, :] = roll(piece, -4 * OWN)[:OWN]
    for t in range(ROWS // LANE):
        at = slice(t * LANE, (t + 1) * LANE)
        for q in range(4):
            acc = jnp.zeros((STRIPE, LANE), f32)
            for d in range(32):
                lo = max(d * OWN, t * LANE)
                hi = min((d + 1) * OWN, (t + 1) * LANE)
                if lo < hi:
                    acc = put(acc, lambda k: wide[d], q * OWN + lo - d * OWN, lo - t * LANE, hi - lo)
            out[q * STRIPE : (q + 1) * STRIPE, at] = acc.astype(bf16)
        out[4 * STRIPE :, at] = rest[at, :].T[:REST].astype(bf16)


def row_block(parts):
    return pl.pallas_call(
        rows_body,
        out_shape=pltpu.VMEM((COLS, ROWS), bf16),
        in_specs=[IN_VMEM],
        out_specs=IN_VMEM,
        scratch_shapes=[
            pltpu.VMEM((32, STRIPE, LANE), f32),
            pltpu.VMEM((ROWS, LANE), f32),
        ],
        name="row_block",
    )(in_vmem(parts))


def pack(master):
    stripes = master[:, : 4 * STRIPE].reshape(OWN, 4, STRIPE).transpose(2, 1, 0).reshape(STRIPE, 4 * OWN)
    rest = jnp.pad(master[:, 4 * STRIPE :], ((0, STRIPE - OWN), (0, 0)))
    return jnp.concatenate([stripes, rest], axis=1)


def unpack(grad):
    stripes = grad[:, : 4 * OWN].reshape(STRIPE, 4, OWN).transpose(2, 1, 0).reshape(OWN, 4 * STRIPE)
    return jnp.concatenate([stripes, grad[:OWN, 4 * OWN :]], axis=1)


def in_vmem(array):
    return pltpu.with_memory_space_constraint(array, pltpu.VMEM)


def exchange(array, axis):
    return lax.all_to_all(array, axis, split_axis=0, concat_axis=0, tiled=True)


def shards(hidden, cotangent, rewards, groups, lengths, master):
    swap = [(0, 1), (1, 0)]
    cot = cotangent.T
    mine = jnp.stack([rewards, groups, lengths])
    chip = lax.all_gather(mine, CORE)
    other = chip[0] + chip[1] - mine
    plane = lax.all_gather(chip[:, :2], X)
    line = plane.transpose(2, 0, 1, 3).reshape(64)
    copies = jnp.broadcast_to(jnp.pad(line, (0, 64)), (32, LANE))
    copies, later_hidden, later_cot = lax.optimization_barrier((copies, hidden, cot))
    seen = exchange(copies, (ZH, ZL))
    other_hidden = lax.ppermute(later_hidden, CORE, swap)
    other_cot = lax.ppermute(later_cot, CORE, swap)
    core = lax.axis_index(CORE).astype(jnp.int32)
    scal = jnp.concatenate([core[None], jnp.stack([mine, other], axis=1).reshape(24)])
    parts = grad_parts(scal, seen, cot, other_cot, hidden, other_hidden)
    parts = x_sum(exchange(parts, X))
    grad, copies = z_sum(exchange(parts, (ZH, ZL)), pack(master[0]))
    block = row_block(exchange(copies, (X, ZL)))
    rollout = lax.all_gather(block, TP)
    rollout = rollout.reshape(4 * COLS, ROWS).T
    return (unpack(grad)[None], rollout[None])


def solution(mesh):
    torus = Mesh(
        mesh.devices.reshape(4, 8, 4, 2, mesh.shape["tp"]),
        (X, ZL, ZH, CORE, TP),
    )
    placed = (
        P(DP_FSDP, None),
        P(DP_FSDP, TP),
        P(DP_FSDP),
        P(DP_FSDP),
        P(DP_FSDP),
        P(FSDP, DP, TP),
    )
    return jax.shard_map(
        shards,
        mesh=torus,
        in_specs=placed,
        out_specs=(P(FSDP, DP, TP), P(FSDP, None, None)),
        check_vma=False,
    )
```

```python
import jax
import jax.numpy as jnp
from jax import lax
from jax.experimental import pallas as pl
from jax.experimental.pallas import tpu as pltpu
from jax.sharding import Mesh
from jax.sharding import PartitionSpec as P


GROUP = 16
X, ZA, ZB, ZH, CORE, TP = "x", "z_half", "z_quad", "z_hi", "core", "tp"
DP = (X, ZA, ZB)
FSDP = (ZH, CORE)
DP_FSDP = (X, ZA, ZB, ZH, CORE)

ROWS = 896
COLS = 144
OWN = 28
PART = 224
STRIPE = 32
REST = 16
LANE = 128
IN_VMEM = pl.BlockSpec(memory_space=pltpu.VMEM)
f32 = jnp.float32
bf16 = jnp.bfloat16


def lane_iota(rows):
    return lax.broadcasted_iota(jnp.int32, (rows, LANE), 1)


def roll(tile, shift):
    shift = shift % LANE
    return tile if shift == 0 else pltpu.roll(tile, shift, 1)


def put(acc, tiles, src, dst, width):
    lane = lane_iota(acc.shape[0])
    done = 0
    while done < width:
        tile, off = divmod(src + done, LANE)
        take = min(LANE - off, width - done)
        at = dst + done
        moved = roll(tiles(tile), at - off)
        acc = jnp.where((lane >= at) & (lane < at + take), moved, acc)
        done += take
    return acc


def grad_body(scal, seen, own_c, oth_c, own_h, oth_h, out, w_own, w_oth, edge):
    step = pl.program_id(0)

    @pl.when(step == 0)
    def _():
        seen_r = seen[:, 0:32].astype(f32)
        seen_g = seen[:, 32:64]
        pos = lax.broadcasted_iota(jnp.int32, (1, LANE), 1)
        for s in range(8):
            hit = seen_g == scal[9 + s]
            total = jnp.sum(jnp.where(hit, seen_r, 0.0), axis=(0, 1), keepdims=True)
            square = jnp.sum(jnp.where(hit, seen_r * seen_r, 0.0), axis=(0, 1), keepdims=True)
            mean = total / GROUP
            var = square / GROUP - mean * mean
            reward = jnp.full((1, 1), scal[1 + s], jnp.int32).astype(f32)
            adv = (reward - mean) / jnp.sqrt(var + 1.0)
            size = jnp.full((1, 1), scal[17 + s], jnp.int32).astype(f32)
            live = jnp.where(pos < scal[17 + s], 1.0, 0.0)
            scale = adv * live / size
            src, dst = (own_c, w_own) if s < 4 else (oth_c, w_oth)
            at = (s % 4) * LANE
            dst[:, at : at + LANE] = (src[:, at : at + LANE].astype(f32) * scale).astype(bf16)

    block = jnp.dot(w_own[...], own_h[...], preferred_element_type=f32)
    block += jnp.dot(w_oth[...], oth_h[...], preferred_element_type=f32)

    def place(j):
        lo, hi = j * PART, (j + 1) * PART
        tiles = lambda k: block[:, k * LANE : (k + 1) * LANE]
        for x in range(4):
            for t in range(lo // LANE, -(-hi // LANE)):
                begin, end = max(lo, t * LANE), min(hi, (t + 1) * LANE)
                acc = edge[x] if t * LANE < lo else jnp.zeros((COLS, LANE), f32)
                acc = put(acc, tiles, x * PART + begin - lo, begin - t * LANE, end - begin)
                if end == (t + 1) * LANE:
                    out[x, :, t * LANE : end] = acc.astype(bf16)
                else:
                    edge[x] = acc

    for j in range(4):
        pl.when(step == j)(lambda j=j: place(j))


def grad_parts(scal, seen, own_c, oth_c, own_h, oth_h):
    tokens = own_h.shape[0]
    half = pl.BlockSpec((tokens, ROWS), lambda j, scal: (0, 2 * j + scal[0]))
    whole = lambda shape: pl.BlockSpec(shape, lambda j, scal: (0,) * len(shape))
    return pl.pallas_call(
        grad_body,
        out_shape=pltpu.VMEM((4, COLS, ROWS), bf16),
        grid_spec=pltpu.PrefetchScalarGridSpec(
            num_scalar_prefetch=1,
            grid=(4,),
            in_specs=[
                IN_VMEM,
                whole(own_c.shape),
                IN_VMEM,
                half,
                half,
            ],
            out_specs=whole((4, COLS, ROWS)),
            scratch_shapes=[
                pltpu.VMEM((COLS, tokens), bf16),
                pltpu.VMEM((COLS, tokens), bf16),
                pltpu.VMEM((4, COLS, LANE), f32),
            ],
        ),
        compiler_params=pltpu.CompilerParams(dimension_semantics=("arbitrary",)),
        name="grad_parts",
    )(scal, in_vmem(seen), own_c, in_vmem(oth_c), own_h, oth_h)


def x_body(parts, out, total, rest):
    for t in range(ROWS // LANE):
        at = slice(t * LANE, (t + 1) * LANE)
        tile = (parts[0, :, at].astype(f32) + parts[1, :, at].astype(f32)) + (
            parts[2, :, at].astype(f32) + parts[3, :, at].astype(f32)
        )
        total[t] = tile
        rest[at, 0:REST] = tile[4 * STRIPE :, :].T
    rest[ROWS:, 0:REST] = jnp.zeros((8, REST), f32)
    lane = lane_iota(STRIPE)
    for j in range(4):
        for z in range(8):
            at = j * PART + z * OWN
            last = roll(rest[at : at + STRIPE], 4 * OWN)
            acc = jnp.where(lane >= 4 * OWN, last, 0.0)
            for q in range(4):
                acc = put(acc, lambda k: total[k, q * STRIPE : (q + 1) * STRIPE], at, q * OWN, OWN)
            half, quad = divmod(z, 4)
            out[quad * 8 + j * 2 + half] = acc.astype(bf16)


def x_sum(parts):
    return pl.pallas_call(
        x_body,
        out_shape=pltpu.VMEM((32, STRIPE, LANE), bf16),
        in_specs=[IN_VMEM],
        out_specs=IN_VMEM,
        scratch_shapes=[
            pltpu.VMEM((ROWS // LANE, COLS, LANE), f32),
            pltpu.VMEM((ROWS + 8, LANE), f32),
        ],
        name="x_sum",
    )(in_vmem(parts))


def quad_body(parts, out):
    for p in range(8):
        total = (parts[p].astype(f32) + parts[8 + p].astype(f32)) + (
            parts[16 + p].astype(f32) + parts[24 + p].astype(f32)
        )
        j, half = divmod(p, 2)
        for to in range(2):
            out[j * 4 + to * 2 + half] = total.astype(bf16)


def quad_sum(parts):
    return pl.pallas_call(
        quad_body,
        out_shape=pltpu.VMEM((16, STRIPE, LANE), bf16),
        in_specs=[IN_VMEM],
        out_specs=IN_VMEM,
        name="quad_sum",
    )(in_vmem(parts))


def z_body(half, parts, mine, other, grad, copies):
    for p in range(2):
        total = [parts[2 * k + p].astype(f32) for k in range(8)]
        while len(total) > 1:
            total = [a + b for a, b in zip(total[::2], total[1::2])]
        own = half[0] == p
        new = (jnp.where(own, mine[...], other[...]) - 0.1 * total[0]).astype(bf16)
        for d in range(16):
            copies[2 * d + p] = new

        @pl.when(own)
        def _():
            grad[...] = total[0]


def z_sum(half, parts, mine, other):
    return pl.pallas_call(
        z_body,
        out_shape=(
            pltpu.VMEM((STRIPE, LANE), f32),
            pltpu.VMEM((32, STRIPE, LANE), bf16),
        ),
        in_specs=[pl.BlockSpec(memory_space=pltpu.SMEM), IN_VMEM, IN_VMEM, IN_VMEM],
        out_specs=(IN_VMEM, IN_VMEM),
        name="z_sum",
    )(half, in_vmem(parts), in_vmem(mine), in_vmem(other))


def rows_body(parts, out, wide, rest):
    for d in range(32):
        x, half, quad = d // 8, d % 8 // 4, d % 4
        piece = parts[(x * 4 + quad) * 2 + half].astype(f32)
        wide[d] = piece
        rest[d * OWN : (d + 1) * OWN, :] = roll(piece, -4 * OWN)[:OWN]
    for t in range(ROWS // LANE):
        at = slice(t * LANE, (t + 1) * LANE)
        for q in range(4):
            acc = jnp.zeros((STRIPE, LANE), f32)
            for d in range(32):
                lo = max(d * OWN, t * LANE)
                hi = min((d + 1) * OWN, (t + 1) * LANE)
                if lo < hi:
                    acc = put(acc, lambda k: wide[d], q * OWN + lo - d * OWN, lo - t * LANE, hi - lo)
            out[q * STRIPE : (q + 1) * STRIPE, at] = acc.astype(bf16)
        out[4 * STRIPE :, at] = rest[at, :].T[:REST].astype(bf16)


def row_block(parts):
    return pl.pallas_call(
        rows_body,
        out_shape=pltpu.VMEM((COLS, ROWS), bf16),
        in_specs=[IN_VMEM],
        out_specs=IN_VMEM,
        scratch_shapes=[
            pltpu.VMEM((32, STRIPE, LANE), f32),
            pltpu.VMEM((ROWS, LANE), f32),
        ],
        name="row_block",
    )(in_vmem(parts))


def pack(master):
    stripes = master[:, : 4 * STRIPE].reshape(OWN, 4, STRIPE).transpose(2, 1, 0).reshape(STRIPE, 4 * OWN)
    rest = jnp.pad(master[:, 4 * STRIPE :], ((0, STRIPE - OWN), (0, 0)))
    return jnp.concatenate([stripes, rest], axis=1)


def unpack(grad):
    stripes = grad[:, : 4 * OWN].reshape(STRIPE, 4, OWN).transpose(2, 1, 0).reshape(OWN, 4 * STRIPE)
    return jnp.concatenate([stripes, grad[:OWN, 4 * OWN :]], axis=1)


def in_vmem(array):
    return pltpu.with_memory_space_constraint(array, pltpu.VMEM)


def exchange(array, axis):
    return lax.all_to_all(array, axis, split_axis=0, concat_axis=0, tiled=True)


def shards(hidden, cotangent, rewards, groups, lengths, master):
    swap = [(0, 1), (1, 0)]
    cot = cotangent.T
    mine = jnp.stack([rewards, groups, lengths])
    chip = lax.all_gather(mine, CORE)
    other = chip[0] + chip[1] - mine
    plane = lax.all_gather(chip[:, :2], X)
    line = plane.transpose(2, 0, 1, 3).reshape(64)
    copies = jnp.broadcast_to(jnp.pad(line, (0, 64)), (32, LANE))
    copies, later_hidden, later_cot, later_master = lax.optimization_barrier((copies, hidden, cot, master))
    packed = pack(later_master[0])
    seen = exchange(copies, (ZH, ZA, ZB))
    other_hidden = lax.ppermute(later_hidden, CORE, swap)
    other_cot = lax.ppermute(later_cot, CORE, swap)
    other_packed = lax.ppermute(packed, ZA, swap)
    core = lax.axis_index(CORE).astype(jnp.int32)
    scal = jnp.concatenate([core[None], jnp.stack([mine, other], axis=1).reshape(24)])
    parts = grad_parts(scal, seen, cot, other_cot, hidden, other_hidden)
    parts = x_sum(exchange(parts, X))
    parts = quad_sum(exchange(parts, ZB))
    half = lax.axis_index(ZA).astype(jnp.int32)[None]
    grad, copies = z_sum(half, exchange(parts, (ZH, ZA)), packed, other_packed)
    block = row_block(exchange(copies, (X, ZB)))
    rollout = lax.all_gather(block, TP)
    rollout = rollout.reshape(4 * COLS, ROWS).T
    return (unpack(grad)[None], rollout[None])


def solution(mesh):
    torus = Mesh(
        mesh.devices.reshape(4, 2, 4, 4, 2, mesh.shape["tp"]),
        (X, ZA, ZB, ZH, CORE, TP),
    )
    placed = (
        P(DP_FSDP, None),
        P(DP_FSDP, TP),
        P(DP_FSDP),
        P(DP_FSDP),
        P(DP_FSDP),
        P(FSDP, DP, TP),
    )
    return jax.shard_map(
        shards,
        mesh=torus,
        in_specs=placed,
        out_specs=(P(FSDP, DP, TP), P(FSDP, None, None)),
        check_vma=False,
    )
```

```python
import jax
import jax.numpy as jnp
from jax import lax
from jax.experimental import pallas as pl
from jax.experimental.pallas import tpu as pltpu
from jax.sharding import Mesh
from jax.sharding import PartitionSpec as P


GROUP = 16
X, ZA, ZB, ZH, CORE, TP = "x", "z_half", "z_quad", "z_hi", "core", "tp"
DP = (X, ZA, ZB)
FSDP = (ZH, CORE)
DP_FSDP = (X, ZA, ZB, ZH, CORE)

ROWS = 896
COLS = 144
OWN = 28
PART = 224
STRIPE = 32
REST = 16
LANE = 128
IN_VMEM = pl.BlockSpec(memory_space=pltpu.VMEM)
f32 = jnp.float32
bf16 = jnp.bfloat16


def lane_iota(rows):
    return lax.broadcasted_iota(jnp.int32, (rows, LANE), 1)


def roll(tile, shift):
    shift = shift % LANE
    return tile if shift == 0 else pltpu.roll(tile, shift, 1)


def put(acc, tiles, src, dst, width):
    lane = lane_iota(acc.shape[0])
    done = 0
    while done < width:
        tile, off = divmod(src + done, LANE)
        take = min(LANE - off, width - done)
        at = dst + done
        moved = roll(tiles(tile), at - off)
        acc = jnp.where((lane >= at) & (lane < at + take), moved, acc)
        done += take
    return acc


def grad_body(scal, seen, own_c, oth_c, own_h, oth_h, out, w_own, w_oth, edge):
    step = pl.program_id(0)

    @pl.when(step == 0)
    def _():
        seen_r = seen[:, 0:32].astype(f32)
        seen_g = seen[:, 32:64]
        pos = lax.broadcasted_iota(jnp.int32, (1, LANE), 1)
        for s in range(8):
            hit = seen_g == scal[9 + s]
            total = jnp.sum(jnp.where(hit, seen_r, 0.0), axis=(0, 1), keepdims=True)
            square = jnp.sum(jnp.where(hit, seen_r * seen_r, 0.0), axis=(0, 1), keepdims=True)
            mean = total / GROUP
            var = square / GROUP - mean * mean
            reward = jnp.full((1, 1), scal[1 + s], jnp.int32).astype(f32)
            adv = (reward - mean) / jnp.sqrt(var + 1.0)
            size = jnp.full((1, 1), scal[17 + s], jnp.int32).astype(f32)
            live = jnp.where(pos < scal[17 + s], 1.0, 0.0)
            scale = adv * live / size
            src, dst = (own_c, w_own) if s < 4 else (oth_c, w_oth)
            at = (s % 4) * LANE
            dst[:, at : at + LANE] = (src[:, at : at + LANE].astype(f32) * scale).astype(bf16)

    block = jnp.dot(w_own[...], own_h[...], preferred_element_type=f32)
    block += jnp.dot(w_oth[...], oth_h[...], preferred_element_type=f32)

    def place(j):
        lo, hi = j * PART, (j + 1) * PART
        tiles = lambda k: block[:, k * LANE : (k + 1) * LANE]
        for x in range(4):
            for t in range(lo // LANE, -(-hi // LANE)):
                begin, end = max(lo, t * LANE), min(hi, (t + 1) * LANE)
                acc = edge[x] if t * LANE < lo else jnp.zeros((COLS, LANE), f32)
                acc = put(acc, tiles, x * PART + begin - lo, begin - t * LANE, end - begin)
                if end == (t + 1) * LANE:
                    out[x, :, t * LANE : end] = acc.astype(bf16)
                else:
                    edge[x] = acc

    for j in range(4):
        pl.when(step == j)(lambda j=j: place(j))


def grad_parts(scal, seen, own_c, oth_c, own_h, oth_h):
    tokens = own_h.shape[0]
    half = pl.BlockSpec((tokens, ROWS), lambda j, scal: (0, 2 * j + scal[0]))
    whole = lambda shape: pl.BlockSpec(shape, lambda j, scal: (0,) * len(shape))
    return pl.pallas_call(
        grad_body,
        out_shape=pltpu.VMEM((4, COLS, ROWS), bf16),
        grid_spec=pltpu.PrefetchScalarGridSpec(
            num_scalar_prefetch=1,
            grid=(4,),
            in_specs=[
                IN_VMEM,
                whole(own_c.shape),
                IN_VMEM,
                half,
                half,
            ],
            out_specs=whole((4, COLS, ROWS)),
            scratch_shapes=[
                pltpu.VMEM((COLS, tokens), bf16),
                pltpu.VMEM((COLS, tokens), bf16),
                pltpu.VMEM((4, COLS, LANE), f32),
            ],
        ),
        compiler_params=pltpu.CompilerParams(dimension_semantics=("arbitrary",)),
        name="grad_parts",
    )(scal, in_vmem(seen), own_c, in_vmem(oth_c), own_h, oth_h)


def x_body(parts, out, total, rest):
    for t in range(ROWS // LANE):
        at = slice(t * LANE, (t + 1) * LANE)
        tile = (parts[0, :, at].astype(f32) + parts[1, :, at].astype(f32)) + (
            parts[2, :, at].astype(f32) + parts[3, :, at].astype(f32)
        )
        total[t] = tile
        rest[at, 0:REST] = tile[4 * STRIPE :, :].T
    rest[ROWS:, 0:REST] = jnp.zeros((8, REST), f32)
    lane = lane_iota(STRIPE)
    for j in range(4):
        for z in range(8):
            at = j * PART + z * OWN
            last = roll(rest[at : at + STRIPE], 4 * OWN)
            acc = jnp.where(lane >= 4 * OWN, last, 0.0)
            for q in range(4):
                acc = put(acc, lambda k: total[k, q * STRIPE : (q + 1) * STRIPE], at, q * OWN, OWN)
            half, quad = divmod(z, 4)
            out[quad * 8 + j * 2 + half] = acc.astype(bf16)


def x_sum(parts):
    return pl.pallas_call(
        x_body,
        out_shape=pltpu.VMEM((32, STRIPE, LANE), bf16),
        in_specs=[IN_VMEM],
        out_specs=IN_VMEM,
        scratch_shapes=[
            pltpu.VMEM((ROWS // LANE, COLS, LANE), f32),
            pltpu.VMEM((ROWS + 8, LANE), f32),
        ],
        name="x_sum",
    )(in_vmem(parts))


def quad_body(parts, out):
    for p in range(8):
        total = (parts[p].astype(f32) + parts[8 + p].astype(f32)) + (
            parts[16 + p].astype(f32) + parts[24 + p].astype(f32)
        )
        j, half = divmod(p, 2)
        for to in range(2):
            out[j * 4 + to * 2 + half] = total.astype(bf16)


def quad_sum(parts):
    return pl.pallas_call(
        quad_body,
        out_shape=pltpu.VMEM((16, STRIPE, LANE), bf16),
        in_specs=[IN_VMEM],
        out_specs=IN_VMEM,
        name="quad_sum",
    )(in_vmem(parts))


def z_body(half, parts, mine, other, grad, copies):
    for p in range(2):
        total = [parts[2 * k + p].astype(f32) for k in range(8)]
        while len(total) > 1:
            total = [a + b for a, b in zip(total[::2], total[1::2])]
        own = half[0] == p
        new = (jnp.where(own, mine[...], other[...]) - 0.1 * total[0]).astype(bf16)
        for d in range(16):
            copies[2 * d + p] = new

        @pl.when(own)
        def _():
            grad[...] = total[0]


def z_sum(half, parts, mine, other):
    return pl.pallas_call(
        z_body,
        out_shape=(
            pltpu.VMEM((STRIPE, LANE), f32),
            pltpu.VMEM((32, STRIPE, LANE), bf16),
        ),
        in_specs=[pl.BlockSpec(memory_space=pltpu.SMEM), IN_VMEM, IN_VMEM, IN_VMEM],
        out_specs=(IN_VMEM, IN_VMEM),
        name="z_sum",
    )(half, in_vmem(parts), in_vmem(mine), in_vmem(other))


def rows_body(parts, out, wide, rest):
    for d in range(32):
        x, half, quad = d // 8, d % 8 // 4, d % 4
        piece = parts[(x * 4 + quad) * 2 + half].astype(f32)
        wide[d] = piece
        rest[d * OWN : (d + 1) * OWN, :] = roll(piece, -4 * OWN)[:OWN]
    for t in range(ROWS // LANE):
        at = slice(t * LANE, (t + 1) * LANE)
        for q in range(4):
            acc = jnp.zeros((STRIPE, LANE), f32)
            for d in range(32):
                lo = max(d * OWN, t * LANE)
                hi = min((d + 1) * OWN, (t + 1) * LANE)
                if lo < hi:
                    acc = put(acc, lambda k: wide[d], q * OWN + lo - d * OWN, lo - t * LANE, hi - lo)
            out[q * STRIPE : (q + 1) * STRIPE, at] = acc.astype(bf16)
        out[4 * STRIPE :, at] = rest[at, :].T[:REST].astype(bf16)


def row_block(parts):
    return pl.pallas_call(
        rows_body,
        out_shape=pltpu.VMEM((COLS, ROWS), bf16),
        in_specs=[IN_VMEM],
        out_specs=IN_VMEM,
        scratch_shapes=[
            pltpu.VMEM((32, STRIPE, LANE), f32),
            pltpu.VMEM((ROWS, LANE), f32),
        ],
        name="row_block",
    )(in_vmem(parts))


def pack(master):
    stripes = master[:, : 4 * STRIPE].reshape(OWN, 4, STRIPE).transpose(2, 1, 0).reshape(STRIPE, 4 * OWN)
    rest = jnp.pad(master[:, 4 * STRIPE :], ((0, STRIPE - OWN), (0, 0)))
    return jnp.concatenate([stripes, rest], axis=1)


def unpack(grad):
    stripes = grad[:, : 4 * OWN].reshape(STRIPE, 4, OWN).transpose(2, 1, 0).reshape(OWN, 4 * STRIPE)
    return jnp.concatenate([stripes, grad[:OWN, 4 * OWN :]], axis=1)


def in_vmem(array):
    return pltpu.with_memory_space_constraint(array, pltpu.VMEM)


def exchange(array, axis):
    return lax.all_to_all(array, axis, split_axis=0, concat_axis=0, tiled=True)


def shards(hidden, cotangent, rewards, groups, lengths, master):
    swap = [(0, 1), (1, 0)]
    cot = cotangent.T
    mine = jnp.concatenate([rewards, groups, lengths])
    plane = lax.all_gather(mine, (X, CORE)).reshape(4, 2, 3, 4)
    row = plane.transpose(2, 0, 1, 3).reshape(3, 32)
    copies = jnp.broadcast_to(jnp.pad(row[:2].reshape(64), (0, 64)), (32, LANE))
    copies, later_hidden, later_cot, later_master = lax.optimization_barrier((copies, hidden, cot, master[0]))
    other_hidden = lax.ppermute(later_hidden, CORE, swap)
    other_cot = lax.ppermute(later_cot, CORE, swap)
    other_master = lax.ppermute(later_master, ZA, swap)
    seen = exchange(copies, (ZH, ZA, ZB))
    core = lax.axis_index(CORE).astype(jnp.int32)
    chip = lax.dynamic_index_in_dim(plane, lax.axis_index(X), 0, keepdims=False)
    other = chip[0] + chip[1] - mine.reshape(3, 4)
    scal = jnp.concatenate([core[None], jnp.stack([mine.reshape(3, 4), other], axis=1).reshape(24)])
    packed, other_packed = pack(later_master), pack(other_master)
    half = lax.axis_index(ZA).astype(jnp.int32)[None]
    seen, packed, other_packed, scal, half = lax.optimization_barrier(
        (seen, packed, other_packed, scal, half)
    )
    parts = grad_parts(scal, seen, cot, other_cot, hidden, other_hidden)
    parts = x_sum(exchange(parts, X))
    parts = quad_sum(exchange(parts, ZB))
    grad, copies = z_sum(half, exchange(parts, (ZH, ZA)), packed, other_packed)
    block = row_block(exchange(copies, (X, ZB)))
    rollout = lax.all_gather(block, TP)
    rollout = rollout.reshape(4 * COLS, ROWS).T
    return (unpack(grad)[None], rollout[None])


def solution(mesh):
    torus = Mesh(
        mesh.devices.reshape(4, 2, 4, 4, 2, mesh.shape["tp"]),
        (X, ZA, ZB, ZH, CORE, TP),
    )
    placed = (
        P(DP_FSDP, None),
        P(DP_FSDP, TP),
        P(DP_FSDP),
        P(DP_FSDP),
        P(DP_FSDP),
        P(FSDP, DP, TP),
    )
    return jax.shard_map(
        shards,
        mesh=torus,
        in_specs=placed,
        out_specs=(P(FSDP, DP, TP), P(FSDP, None, None)),
        check_vma=False,
    )
```

```python
import jax
import jax.numpy as jnp
from jax import lax
from jax.experimental import pallas as pl
from jax.experimental.pallas import tpu as pltpu
from jax.sharding import Mesh
from jax.sharding import PartitionSpec as P


GROUP = 16
X, ZA, ZB, ZH, CORE, TP = "x", "z_half", "z_quad", "z_hi", "core", "tp"
DP = (X, ZA, ZB)
FSDP = (ZH, CORE)
DP_FSDP = (X, ZA, ZB, ZH, CORE)

ROWS = 896
COLS = 144
OWN = 28
PART = 224
STRIPE = 32
REST = 16
LANE = 128
INFO = 12
IN_VMEM = pl.BlockSpec(memory_space=pltpu.VMEM)
f32 = jnp.float32
bf16 = jnp.bfloat16


def lane_iota(rows):
    return lax.broadcasted_iota(jnp.int32, (rows, LANE), 1)


def roll(tile, shift):
    shift = shift % LANE
    return tile if shift == 0 else pltpu.roll(tile, shift, 1)


def put(acc, tiles, src, dst, width):
    lane = lane_iota(acc.shape[0])
    done = 0
    while done < width:
        tile, off = divmod(src + done, LANE)
        take = min(LANE - off, width - done)
        at = dst + done
        moved = roll(tiles(tile), at - off)
        acc = jnp.where((lane >= at) & (lane < at + take), moved, acc)
        done += take
    return acc


def grad_body(place_at, x_at, info, seen, own_c, oth_c, own_h, oth_h, out, w_own, w_oth, edge):
    step = pl.program_id(0)

    @pl.when(step == 0)
    def _():
        lane = lane_iota(seen.shape[0])
        rewards = jnp.where((lane < 8 * INFO) & (lane % INFO < 4), seen[...], 0).astype(f32)
        labels = roll(seen[...], -4)
        pos = lax.broadcasted_iota(jnp.int32, (1, LANE), 1)
        for s in range(8):
            core = place_at[0] % 2 if s < 4 else 1 - place_at[0] % 2
            base = (x_at[0] * 2 + core) * INFO + s % 4
            reward, label, length = info[base], info[base + 4], info[base + 8]
            mates = jnp.where(labels == label, rewards, 0.0)
            total = jnp.sum(mates, axis=(0, 1), keepdims=True)
            square = jnp.sum(mates * mates, axis=(0, 1), keepdims=True)
            mean = total / GROUP
            var = square / GROUP - mean * mean
            adv = (jnp.full((1, 1), reward, jnp.int32).astype(f32) - mean) / jnp.sqrt(var + 1.0)
            live = jnp.where(pos < length, 1.0, 0.0)
            scale = adv * live / jnp.full((1, 1), length, jnp.int32).astype(f32)
            src, dst = (own_c, w_own) if s < 4 else (oth_c, w_oth)
            at = (s % 4) * LANE
            dst[:, at : at + LANE] = (src[:, at : at + LANE].astype(f32) * scale).astype(bf16)

    block = jnp.dot(w_own[...], own_h[...], preferred_element_type=f32)
    block += jnp.dot(w_oth[...], oth_h[...], preferred_element_type=f32)

    def place(j):
        lo, hi = j * PART, (j + 1) * PART
        tiles = lambda k: block[:, k * LANE : (k + 1) * LANE]
        for x in range(4):
            for t in range(lo // LANE, -(-hi // LANE)):
                begin, end = max(lo, t * LANE), min(hi, (t + 1) * LANE)
                acc = edge[x] if t * LANE < lo else jnp.zeros((COLS, LANE), f32)
                acc = put(acc, tiles, x * PART + begin - lo, begin - t * LANE, end - begin)
                if end == (t + 1) * LANE:
                    out[x, :, t * LANE : end] = acc.astype(bf16)
                else:
                    edge[x] = acc

    for j in range(4):
        pl.when(step == j)(lambda j=j: place(j))


def grad_parts(place_at, x_at, info, seen, own_c, oth_c, own_h, oth_h):
    tokens = own_h.shape[0]
    half = pl.BlockSpec((tokens, ROWS), lambda j, place, x, info: (0, 2 * j + place[0] % 2))
    whole = lambda shape: pl.BlockSpec(shape, lambda j, place, x, info: (0,) * len(shape))
    return pl.pallas_call(
        grad_body,
        out_shape=pltpu.VMEM((4, COLS, ROWS), bf16),
        grid_spec=pltpu.PrefetchScalarGridSpec(
            num_scalar_prefetch=3,
            grid=(4,),
            in_specs=[
                IN_VMEM,
                whole(own_c.shape),
                IN_VMEM,
                half,
                half,
            ],
            out_specs=whole((4, COLS, ROWS)),
            scratch_shapes=[
                pltpu.VMEM((COLS, tokens), bf16),
                pltpu.VMEM((COLS, tokens), bf16),
                pltpu.VMEM((4, COLS, LANE), f32),
            ],
        ),
        compiler_params=pltpu.CompilerParams(dimension_semantics=("arbitrary",)),
        name="grad_parts",
    )(place_at, x_at, info, in_vmem(seen), own_c, in_vmem(oth_c), own_h, oth_h)


def x_body(parts, out, total, rest):
    for t in range(ROWS // LANE):
        at = slice(t * LANE, (t + 1) * LANE)
        tile = (parts[0, :, at].astype(f32) + parts[1, :, at].astype(f32)) + (
            parts[2, :, at].astype(f32) + parts[3, :, at].astype(f32)
        )
        total[t] = tile
        rest[at, 0:REST] = tile[4 * STRIPE :, :].T
    rest[ROWS:, 0:REST] = jnp.zeros((8, REST), f32)
    lane = lane_iota(STRIPE)
    for j in range(4):
        for z in range(8):
            at = j * PART + z * OWN
            last = roll(rest[at : at + STRIPE], 4 * OWN)
            acc = jnp.where(lane >= 4 * OWN, last, 0.0)
            for q in range(4):
                acc = put(acc, lambda k: total[k, q * STRIPE : (q + 1) * STRIPE], at, q * OWN, OWN)
            half, quad = divmod(z, 4)
            out[quad * 8 + j * 2 + half] = acc.astype(bf16)


def x_sum(parts):
    return pl.pallas_call(
        x_body,
        out_shape=pltpu.VMEM((32, STRIPE, LANE), bf16),
        in_specs=[IN_VMEM],
        out_specs=IN_VMEM,
        scratch_shapes=[
            pltpu.VMEM((ROWS // LANE, COLS, LANE), f32),
            pltpu.VMEM((ROWS + 8, LANE), f32),
        ],
        name="x_sum",
    )(in_vmem(parts))


def quad_body(parts, out):
    for p in range(8):
        total = (parts[p].astype(f32) + parts[8 + p].astype(f32)) + (
            parts[16 + p].astype(f32) + parts[24 + p].astype(f32)
        )
        j, half = divmod(p, 2)
        for to in range(2):
            out[j * 4 + to * 2 + half] = total.astype(bf16)


def quad_sum(parts):
    return pl.pallas_call(
        quad_body,
        out_shape=pltpu.VMEM((16, STRIPE, LANE), bf16),
        in_specs=[IN_VMEM],
        out_specs=IN_VMEM,
        name="quad_sum",
    )(in_vmem(parts))


def packed(master, wide, tall):
    wide[0:OWN, 0:COLS] = master[:, 0, :]
    tall[0:OWN] = wide[0:OWN, 0:LANE]
    stripes = tall[...].T
    lane = lane_iota(STRIPE)
    acc = jnp.where(lane >= 4 * OWN, roll(wide[:, LANE:], 4 * OWN), 0.0)
    for q in range(4):
        acc = put(acc, lambda k: stripes[q * STRIPE : (q + 1) * STRIPE], 0, q * OWN, OWN)
    return acc


def z_body(place_at, parts, mine, other, grad, copies, wide, tall):
    wide[...] = jnp.zeros(wide.shape, f32)
    tall[...] = jnp.zeros(tall.shape, f32)
    masters = packed(mine, wide, tall), packed(other, wide, tall)
    for p in range(2):
        total = [parts[2 * k + p].astype(f32) for k in range(8)]
        while len(total) > 1:
            total = [a + b for a, b in zip(total[::2], total[1::2])]
        own = place_at[0] // 2 == p
        new = (jnp.where(own, *masters) - 0.1 * total[0]).astype(bf16)
        for d in range(16):
            copies[2 * d + p] = new

        @pl.when(own)
        def _():
            for q in range(4):
                tall[q * STRIPE : (q + 1) * STRIPE] = roll(total[0], -q * OWN)
            grad[:, 0, 0:LANE] = tall[...].T[:OWN]
            grad[:, 0, LANE:COLS] = roll(total[0], -4 * OWN)[:OWN, : COLS - LANE]


def z_sum(place_at, parts, mine, other):
    return pl.pallas_call(
        z_body,
        out_shape=(
            pltpu.VMEM((OWN, 1, COLS), f32),
            pltpu.VMEM((32, STRIPE, LANE), bf16),
        ),
        in_specs=[pl.BlockSpec(memory_space=pltpu.SMEM), IN_VMEM, IN_VMEM, IN_VMEM],
        out_specs=(IN_VMEM, IN_VMEM),
        scratch_shapes=[pltpu.VMEM((STRIPE, 2 * LANE), f32), pltpu.VMEM((LANE, LANE), f32)],
        name="z_sum",
    )(place_at, in_vmem(parts), in_vmem(mine), in_vmem(other))


def rows_body(parts, out, wide, rest):
    for d in range(32):
        x, half, quad = d // 8, d % 8 // 4, d % 4
        piece = parts[(x * 4 + quad) * 2 + half].astype(f32)
        wide[d] = piece
        rest[d * OWN : (d + 1) * OWN, :] = roll(piece, -4 * OWN)[:OWN]
    for t in range(ROWS // LANE):
        at = slice(t * LANE, (t + 1) * LANE)
        for q in range(4):
            acc = jnp.zeros((STRIPE, LANE), f32)
            for d in range(32):
                lo = max(d * OWN, t * LANE)
                hi = min((d + 1) * OWN, (t + 1) * LANE)
                if lo < hi:
                    acc = put(acc, lambda k: wide[d], q * OWN + lo - d * OWN, lo - t * LANE, hi - lo)
            out[q * STRIPE : (q + 1) * STRIPE, at] = acc.astype(bf16)
        out[4 * STRIPE :, at] = rest[at, :].T[:REST].astype(bf16)


def row_block(parts):
    return pl.pallas_call(
        rows_body,
        out_shape=pltpu.VMEM((COLS, ROWS), bf16),
        in_specs=[IN_VMEM],
        out_specs=IN_VMEM,
        scratch_shapes=[
            pltpu.VMEM((32, STRIPE, LANE), f32),
            pltpu.VMEM((ROWS, LANE), f32),
        ],
        name="row_block",
    )(in_vmem(parts))


def in_vmem(array):
    return pltpu.with_memory_space_constraint(array, pltpu.VMEM)


def exchange(array, axis):
    return lax.all_to_all(array, axis, split_axis=0, concat_axis=0, tiled=True)


def shards(hidden, cotangent, rewards, groups, lengths, master):
    swap = [(0, 1), (1, 0)]
    cot = cotangent.T
    core, x, half = (lax.axis_index(name).astype(jnp.int32) for name in (CORE, X, ZA))
    place_at = half * 2 + core
    base = (x * 2 + place_at % 2) * INFO
    mine = jnp.concatenate([rewards, groups, lengths])
    info = lax.dynamic_update_slice(jnp.zeros(LANE, jnp.int32), mine, (base,))
    info = lax.psum(info, (X, CORE))
    copies = jnp.broadcast_to(info, (32, LANE))
    copies, later_hidden, later_cot, info = lax.optimization_barrier((copies, hidden, cot, info))
    other_hidden = lax.ppermute(later_hidden, CORE, swap)
    other_cot = lax.ppermute(later_cot, CORE, swap)
    seen = exchange(copies, (ZH, ZA, ZB))
    parts = grad_parts(place_at[None], x[None], info, seen, cot, other_cot, hidden, other_hidden)
    parts, later_master = lax.optimization_barrier((parts, master.transpose(1, 0, 2)))
    parts = exchange(parts, X)
    other_master = lax.ppermute(later_master, ZA, swap)
    parts, later_master, other_master = lax.optimization_barrier((parts, later_master, other_master))
    parts = quad_sum(exchange(x_sum(parts), ZB))
    grad, copies = z_sum(place_at[None], exchange(parts, (ZH, ZA)), later_master, other_master)
    block = row_block(exchange(copies, (X, ZB)))
    block, grad = lax.optimization_barrier((block, grad))
    rollout = lax.all_gather(block, TP)
    rollout = rollout.reshape(4 * COLS, ROWS).T
    return (grad.transpose(1, 0, 2), rollout[None])


def solution(mesh):
    torus = Mesh(
        mesh.devices.reshape(4, 2, 4, 4, 2, mesh.shape["tp"]),
        (X, ZA, ZB, ZH, CORE, TP),
    )
    placed = (
        P(DP_FSDP, None),
        P(DP_FSDP, TP),
        P(DP_FSDP),
        P(DP_FSDP),
        P(DP_FSDP),
        P(FSDP, DP, TP),
    )
    return jax.shard_map(
        shards,
        mesh=torus,
        in_specs=placed,
        out_specs=(P(FSDP, DP, TP), P(FSDP, None, None)),
        check_vma=False,
    )
```

```python
import jax
import jax.numpy as jnp
from jax import lax
from jax.experimental import pallas as pl
from jax.experimental.pallas import tpu as pltpu
from jax.sharding import Mesh
from jax.sharding import PartitionSpec as P


GROUP = 16
X, ZA, ZB, ZH, CORE, TP = "x", "z_half", "z_quad", "z_hi", "core", "tp"
DP = (X, ZA, ZB)
FSDP = (ZH, CORE)
DP_FSDP = (X, ZA, ZB, ZH, CORE)

ROWS = 896
COLS = 144
OWN = 28
PART = 224
STRIPE = 32
REST = 16
LANE = 128
INFO = 12
IN_VMEM = pl.BlockSpec(memory_space=pltpu.VMEM)
f32 = jnp.float32
bf16 = jnp.bfloat16


def lane_iota(rows):
    return lax.broadcasted_iota(jnp.int32, (rows, LANE), 1)


def roll(tile, shift):
    shift = shift % LANE
    return tile if shift == 0 else pltpu.roll(tile, shift, 1)


def put(acc, tiles, src, dst, width):
    lane = lane_iota(acc.shape[0])
    done = 0
    while done < width:
        tile, off = divmod(src + done, LANE)
        take = min(LANE - off, width - done)
        at = dst + done
        moved = roll(tiles(tile), at - off)
        acc = jnp.where((lane >= at) & (lane < at + take), moved, acc)
        done += take
    return acc


def grad_body(place_at, x_at, info, seen, own_c, oth_c, own_h, oth_h, out, w_own, w_oth, edge):
    step = pl.program_id(0)

    @pl.when(step == 0)
    def _():
        lane = lane_iota(seen.shape[0])
        rewards = jnp.where((lane < 8 * INFO) & (lane % INFO < 4), seen[...], 0).astype(f32)
        labels = roll(seen[...], -4)
        pos = lax.broadcasted_iota(jnp.int32, (1, LANE), 1)
        for s in range(8):
            core = place_at[0] % 2 if s < 4 else 1 - place_at[0] % 2
            base = (x_at[0] * 2 + core) * INFO + s % 4
            reward, label, length = info[base], info[base + 4], info[base + 8]
            mates = jnp.where(labels == label, rewards, 0.0)
            total = jnp.sum(mates, axis=(0, 1), keepdims=True)
            square = jnp.sum(mates * mates, axis=(0, 1), keepdims=True)
            mean = total / GROUP
            var = square / GROUP - mean * mean
            adv = (jnp.full((1, 1), reward, jnp.int32).astype(f32) - mean) / jnp.sqrt(var + 1.0)
            live = jnp.where(pos < length, 1.0, 0.0)
            scale = adv * live / jnp.full((1, 1), length, jnp.int32).astype(f32)
            src, dst = (own_c, w_own) if s < 4 else (oth_c, w_oth)
            at = (s % 4) * LANE
            dst[:, at : at + LANE] = (src[:, at : at + LANE].astype(f32) * scale).astype(bf16)

    block = jnp.dot(w_own[...], own_h[...], preferred_element_type=f32)
    at = pl.multiple_of((2 * step + place_at[0] % 2) * ROWS, LANE)
    block += jnp.dot(w_oth[...], oth_h[:, pl.ds(at, ROWS)], preferred_element_type=f32)

    def place(j):
        lo, hi = j * PART, (j + 1) * PART
        tiles = lambda k: block[:, k * LANE : (k + 1) * LANE]
        for x in range(4):
            for t in range(lo // LANE, -(-hi // LANE)):
                begin, end = max(lo, t * LANE), min(hi, (t + 1) * LANE)
                acc = edge[x] if t * LANE < lo else jnp.zeros((COLS, LANE), f32)
                acc = put(acc, tiles, x * PART + begin - lo, begin - t * LANE, end - begin)
                if end == (t + 1) * LANE:
                    out[x, :, t * LANE : end] = acc.astype(bf16)
                else:
                    edge[x] = acc

    for j in range(4):
        pl.when(step == j)(lambda j=j: place(j))


def grad_parts(place_at, x_at, info, seen, own_c, oth_c, own_h, oth_h):
    tokens = own_h.shape[0]
    half = pl.BlockSpec((tokens, ROWS), lambda j, place, x, info: (0, 2 * j + place[0] % 2))
    whole = lambda shape: pl.BlockSpec(shape, lambda j, place, x, info: (0,) * len(shape))
    return pl.pallas_call(
        grad_body,
        out_shape=pltpu.VMEM((4, COLS, ROWS), bf16),
        grid_spec=pltpu.PrefetchScalarGridSpec(
            num_scalar_prefetch=3,
            grid=(4,),
            in_specs=[
                IN_VMEM,
                whole(own_c.shape),
                IN_VMEM,
                half,
                IN_VMEM,
            ],
            out_specs=whole((4, COLS, ROWS)),
            scratch_shapes=[
                pltpu.VMEM((COLS, tokens), bf16),
                pltpu.VMEM((COLS, tokens), bf16),
                pltpu.VMEM((4, COLS, LANE), f32),
            ],
        ),
        compiler_params=pltpu.CompilerParams(
            dimension_semantics=("arbitrary",), vmem_limit_bytes=24 << 20
        ),
        name="grad_parts",
    )(place_at, x_at, info, in_vmem(seen), in_hbm(own_c), in_vmem(oth_c), in_hbm(own_h), in_vmem(oth_h))


def x_body(parts, out, total, rest):
    for t in range(ROWS // LANE):
        at = slice(t * LANE, (t + 1) * LANE)
        tile = (parts[0, :, at].astype(f32) + parts[1, :, at].astype(f32)) + (
            parts[2, :, at].astype(f32) + parts[3, :, at].astype(f32)
        )
        total[t] = tile
        rest[at, 0:REST] = tile[4 * STRIPE :, :].T
    rest[ROWS:, 0:REST] = jnp.zeros((8, REST), f32)
    lane = lane_iota(STRIPE)
    for j in range(4):
        for z in range(8):
            at = j * PART + z * OWN
            last = roll(rest[at : at + STRIPE], 4 * OWN)
            acc = jnp.where(lane >= 4 * OWN, last, 0.0)
            for q in range(4):
                acc = put(acc, lambda k: total[k, q * STRIPE : (q + 1) * STRIPE], at, q * OWN, OWN)
            half, quad = divmod(z, 4)
            out[quad * 8 + j * 2 + half] = acc.astype(bf16)


def x_sum(parts):
    return pl.pallas_call(
        x_body,
        out_shape=pltpu.VMEM((32, STRIPE, LANE), bf16),
        in_specs=[IN_VMEM],
        out_specs=IN_VMEM,
        scratch_shapes=[
            pltpu.VMEM((ROWS // LANE, COLS, LANE), f32),
            pltpu.VMEM((ROWS + 8, LANE), f32),
        ],
        name="x_sum",
    )(in_vmem(parts))


def quad_body(parts, out):
    for p in range(8):
        total = (parts[p].astype(f32) + parts[8 + p].astype(f32)) + (
            parts[16 + p].astype(f32) + parts[24 + p].astype(f32)
        )
        j, half = divmod(p, 2)
        for to in range(2):
            out[j * 4 + to * 2 + half] = total.astype(bf16)


def quad_sum(parts):
    return pl.pallas_call(
        quad_body,
        out_shape=pltpu.VMEM((16, STRIPE, LANE), bf16),
        in_specs=[IN_VMEM],
        out_specs=IN_VMEM,
        name="quad_sum",
    )(in_vmem(parts))


def packed(master, wide, tall):
    wide[0:OWN, 0:COLS] = master[:, 0, :]
    tall[0:OWN] = wide[0:OWN, 0:LANE]
    stripes = tall[...].T
    lane = lane_iota(STRIPE)
    acc = jnp.where(lane >= 4 * OWN, roll(wide[:, LANE:], 4 * OWN), 0.0)
    for q in range(4):
        acc = put(acc, lambda k: stripes[q * STRIPE : (q + 1) * STRIPE], 0, q * OWN, OWN)
    return acc


def z_body(place_at, parts, mine, other, grad, copies, wide, tall):
    wide[...] = jnp.zeros(wide.shape, f32)
    tall[...] = jnp.zeros(tall.shape, f32)
    masters = packed(mine, wide, tall), packed(other, wide, tall)
    for p in range(2):
        total = [parts[2 * k + p].astype(f32) for k in range(8)]
        while len(total) > 1:
            total = [a + b for a, b in zip(total[::2], total[1::2])]
        own = place_at[0] // 2 == p
        new = (jnp.where(own, *masters) - 0.1 * total[0]).astype(bf16)
        for d in range(16):
            copies[2 * d + p] = new

        @pl.when(own)
        def _():
            for q in range(4):
                tall[q * STRIPE : (q + 1) * STRIPE] = roll(total[0], -q * OWN)
            grad[:, 0, 0:LANE] = tall[...].T[:OWN]
            grad[:, 0, LANE:COLS] = roll(total[0], -4 * OWN)[:OWN, : COLS - LANE]


def z_sum(place_at, parts, mine, other):
    return pl.pallas_call(
        z_body,
        out_shape=(
            pltpu.VMEM((OWN, 1, COLS), f32),
            pltpu.VMEM((32, STRIPE, LANE), bf16),
        ),
        in_specs=[pl.BlockSpec(memory_space=pltpu.SMEM), IN_VMEM, IN_VMEM, IN_VMEM],
        out_specs=(IN_VMEM, IN_VMEM),
        scratch_shapes=[pltpu.VMEM((STRIPE, 2 * LANE), f32), pltpu.VMEM((LANE, LANE), f32)],
        name="z_sum",
    )(place_at, in_vmem(parts), in_vmem(mine), in_vmem(other))


def rows_body(parts, out, wide, rest):
    for d in range(32):
        x, half, quad = d // 8, d % 8 // 4, d % 4
        piece = parts[(x * 4 + quad) * 2 + half].astype(f32)
        wide[d] = piece
        rest[d * OWN : (d + 1) * OWN, :] = roll(piece, -4 * OWN)[:OWN]
    for t in range(ROWS // LANE):
        at = slice(t * LANE, (t + 1) * LANE)
        for q in range(4):
            acc = jnp.zeros((STRIPE, LANE), f32)
            for d in range(32):
                lo = max(d * OWN, t * LANE)
                hi = min((d + 1) * OWN, (t + 1) * LANE)
                if lo < hi:
                    acc = put(acc, lambda k: wide[d], q * OWN + lo - d * OWN, lo - t * LANE, hi - lo)
            out[q * STRIPE : (q + 1) * STRIPE, at] = acc.astype(bf16)
        out[4 * STRIPE :, at] = rest[at, :].T[:REST].astype(bf16)


def row_block(parts):
    return pl.pallas_call(
        rows_body,
        out_shape=pltpu.VMEM((COLS, ROWS), bf16),
        in_specs=[IN_VMEM],
        out_specs=IN_VMEM,
        scratch_shapes=[
            pltpu.VMEM((32, STRIPE, LANE), f32),
            pltpu.VMEM((ROWS, LANE), f32),
        ],
        name="row_block",
    )(in_vmem(parts))


def in_vmem(array):
    return pltpu.with_memory_space_constraint(array, pltpu.VMEM)


def in_hbm(array):
    return pltpu.with_memory_space_constraint(array, pltpu.HBM)


def exchange(array, axis):
    return lax.all_to_all(array, axis, split_axis=0, concat_axis=0, tiled=True)


def shards(hidden, cotangent, rewards, groups, lengths, master):
    swap = [(0, 1), (1, 0)]
    cot = cotangent.T
    core, x, half = (lax.axis_index(name).astype(jnp.int32) for name in (CORE, X, ZA))
    place_at = half * 2 + core
    base = (x * 2 + place_at % 2) * INFO
    mine = jnp.concatenate([rewards, groups, lengths])
    info = lax.dynamic_update_slice(jnp.zeros(LANE, jnp.int32), mine, (base,))
    info = lax.psum(info, (X, CORE))
    copies = jnp.broadcast_to(info, (32, LANE))
    copies, later_hidden, later_cot, info = lax.optimization_barrier((copies, hidden, cot, info))
    other_hidden = lax.ppermute(later_hidden, CORE, swap)
    other_cot = lax.ppermute(later_cot, CORE, swap)
    seen = exchange(copies, (ZH, ZA, ZB))
    parts = grad_parts(place_at[None], x[None], info, seen, cot, other_cot, hidden, other_hidden)
    parts, later_master = lax.optimization_barrier((parts, master.transpose(1, 0, 2)))
    parts = exchange(parts, X)
    other_master = lax.ppermute(later_master, ZA, swap)
    parts, later_master, other_master = lax.optimization_barrier((parts, later_master, other_master))
    parts = quad_sum(exchange(x_sum(parts), ZB))
    grad, copies = z_sum(place_at[None], exchange(parts, (ZH, ZA)), later_master, other_master)
    block = row_block(exchange(copies, (X, ZB)))
    block, grad = lax.optimization_barrier((block, grad))
    rollout = lax.all_gather(block.T[None], TP, axis=2, tiled=True)
    return (grad.transpose(1, 0, 2), rollout)


def solution(mesh):
    torus = Mesh(
        mesh.devices.reshape(4, 2, 4, 4, 2, mesh.shape["tp"]),
        (X, ZA, ZB, ZH, CORE, TP),
    )
    placed = (
        P(DP_FSDP, None),
        P(DP_FSDP, TP),
        P(DP_FSDP),
        P(DP_FSDP),
        P(DP_FSDP),
        P(FSDP, DP, TP),
    )
    return jax.shard_map(
        shards,
        mesh=torus,
        in_specs=placed,
        out_specs=(P(FSDP, DP, TP), P(FSDP, None, None)),
        check_vma=False,
    )
```

```python
import jax
import jax.numpy as jnp
from jax import lax
from jax.experimental import pallas as pl
from jax.experimental.pallas import tpu as pltpu
from jax.sharding import Mesh
from jax.sharding import PartitionSpec as P


GROUP = 16
X, ZA, ZB, ZH, CORE, TP = "x", "z_half", "z_quad", "z_hi", "core", "tp"
DP = (X, ZA, ZB)
FSDP = (ZH, CORE)
DP_FSDP = (X, ZA, ZB, ZH, CORE)

ROWS = 896
COLS = 144
OWN = 28
PART = 224
STRIPE = 32
REST = 16
LANE = 128
INFO = 12
IN_VMEM = pl.BlockSpec(memory_space=pltpu.VMEM)
f32 = jnp.float32
bf16 = jnp.bfloat16


def lane_iota(rows):
    return lax.broadcasted_iota(jnp.int32, (rows, LANE), 1)


def roll(tile, shift):
    shift = shift % LANE
    return tile if shift == 0 else pltpu.roll(tile, shift, 1)


def put(acc, tiles, src, dst, width):
    lane = lane_iota(acc.shape[0])
    done = 0
    while done < width:
        tile, off = divmod(src + done, LANE)
        take = min(LANE - off, width - done)
        at = dst + done
        moved = roll(tiles(tile), at - off)
        acc = jnp.where((lane >= at) & (lane < at + take), moved, acc)
        done += take
    return acc


def grad_body(place_at, x_at, info, seen, own_c, oth_c, own_h, oth_h, out, cot, wide, w_own, w_oth, edge, sems):
    def column(j):
        return pl.ds(pl.multiple_of((2 * j + place_at[0] % 2) * ROWS, LANE), ROWS)

    copies = [pltpu.make_async_copy(own_c, cot, sems.at[4])]
    copies += [pltpu.make_async_copy(own_h.at[:, column(j)], wide.at[j], sems.at[j]) for j in range(4)]
    for copy in copies:
        copy.start()

    lane = lane_iota(seen.shape[0])
    rewards = jnp.where((lane < 8 * INFO) & (lane % INFO < 4), seen[...], 0).astype(f32)
    labels = roll(seen[...], -4)
    row = lax.broadcasted_iota(jnp.int32, (8, LANE), 0)
    pos = lax.broadcasted_iota(jnp.int32, (8, LANE), 1)
    totals, squares = jnp.zeros((8, LANE), f32), jnp.zeros((8, LANE), f32)
    reward, length = jnp.zeros((8, LANE), jnp.int32), jnp.ones((8, LANE), jnp.int32)
    for s in range(8):
        core = place_at[0] % 2 if s < 4 else 1 - place_at[0] % 2
        base = (x_at[0] * 2 + core) * INFO + s % 4
        mates = jnp.where(labels == info[base + 4], rewards, 0.0)
        totals = jnp.where(row == s, jnp.sum(mates, axis=0, keepdims=True), totals)
        squares = jnp.where(row == s, jnp.sum(mates * mates, axis=0, keepdims=True), squares)
        reward = jnp.where(row == s, info[base], reward)
        length = jnp.where(row == s, info[base + 8], length)
    mean = jnp.sum(totals, axis=1, keepdims=True) / GROUP
    var = jnp.sum(squares, axis=1, keepdims=True) / GROUP - mean * mean
    adv = (reward.astype(f32) - mean) / jnp.sqrt(var + 1.0)
    scale = adv * jnp.where(pos < length, 1.0, 0.0) / length.astype(f32)
    copies[0].wait()
    for s in range(8):
        src, dst = (cot, w_own) if s < 4 else (oth_c, w_oth)
        at = (s % 4) * LANE
        dst[:, at : at + LANE] = (src[:, at : at + LANE].astype(f32) * scale[s : s + 1]).astype(bf16)

    def place(j, block):
        lo, hi = j * PART, (j + 1) * PART
        tiles = lambda k: block[:, k * LANE : (k + 1) * LANE]
        for x in range(4):
            for t in range(lo // LANE, -(-hi // LANE)):
                begin, end = max(lo, t * LANE), min(hi, (t + 1) * LANE)
                acc = edge[x] if t * LANE < lo else jnp.zeros((COLS, LANE), f32)
                acc = put(acc, tiles, x * PART + begin - lo, begin - t * LANE, end - begin)
                if end == (t + 1) * LANE:
                    out[x, :, t * LANE : end] = acc.astype(bf16)
                else:
                    edge[x] = acc

    for j in range(4):
        other = jnp.dot(w_oth[...], oth_h[:, column(j)], preferred_element_type=f32)
        copies[1 + j].wait()
        place(j, jnp.dot(w_own[...], wide[j], preferred_element_type=f32) + other)


def grad_parts(place_at, x_at, info, seen, own_c, oth_c, own_h, oth_h):
    tokens = own_h.shape[0]
    scalars = pl.BlockSpec(memory_space=pltpu.SMEM)
    in_place = pl.BlockSpec(memory_space=pl.ANY)
    return pl.pallas_call(
        grad_body,
        out_shape=pltpu.VMEM((4, COLS, ROWS), bf16),
        in_specs=[scalars, scalars, scalars, IN_VMEM, in_place, IN_VMEM, in_place, IN_VMEM],
        out_specs=IN_VMEM,
        scratch_shapes=[
            pltpu.VMEM((COLS, tokens), bf16),
            pltpu.VMEM((4, tokens, ROWS), bf16),
            pltpu.VMEM((COLS, tokens), bf16),
            pltpu.VMEM((COLS, tokens), bf16),
            pltpu.VMEM((4, COLS, LANE), f32),
            pltpu.SemaphoreType.DMA((5,)),
        ],
        compiler_params=pltpu.CompilerParams(vmem_limit_bytes=24 << 20),
        name="grad_parts",
    )(place_at, x_at, info, in_vmem(seen), in_hbm(own_c), in_vmem(oth_c), in_hbm(own_h), in_vmem(oth_h))


def x_body(parts, out, total, rest):
    for t in range(ROWS // LANE):
        at = slice(t * LANE, (t + 1) * LANE)
        tile = (parts[0, :, at].astype(f32) + parts[1, :, at].astype(f32)) + (
            parts[2, :, at].astype(f32) + parts[3, :, at].astype(f32)
        )
        total[t] = tile
        rest[at, 0:REST] = tile[4 * STRIPE :, :].T
    rest[ROWS:, 0:REST] = jnp.zeros((8, REST), f32)
    lane = lane_iota(STRIPE)
    for j in range(4):
        for z in range(8):
            at = j * PART + z * OWN
            last = roll(rest[at : at + STRIPE], 4 * OWN)
            acc = jnp.where(lane >= 4 * OWN, last, 0.0)
            for q in range(4):
                acc = put(acc, lambda k: total[k, q * STRIPE : (q + 1) * STRIPE], at, q * OWN, OWN)
            half, quad = divmod(z, 4)
            out[quad * 8 + j * 2 + half] = acc.astype(bf16)


def x_sum(parts):
    return pl.pallas_call(
        x_body,
        out_shape=pltpu.VMEM((32, STRIPE, LANE), bf16),
        in_specs=[IN_VMEM],
        out_specs=IN_VMEM,
        scratch_shapes=[
            pltpu.VMEM((ROWS // LANE, COLS, LANE), f32),
            pltpu.VMEM((ROWS + 8, LANE), f32),
        ],
        name="x_sum",
    )(in_vmem(parts))


def quad_body(parts, out):
    for p in range(8):
        total = (parts[p].astype(f32) + parts[8 + p].astype(f32)) + (
            parts[16 + p].astype(f32) + parts[24 + p].astype(f32)
        )
        j, half = divmod(p, 2)
        for to in range(2):
            out[j * 4 + to * 2 + half] = total.astype(bf16)


def quad_sum(parts):
    return pl.pallas_call(
        quad_body,
        out_shape=pltpu.VMEM((16, STRIPE, LANE), bf16),
        in_specs=[IN_VMEM],
        out_specs=IN_VMEM,
        name="quad_sum",
    )(in_vmem(parts))


def packed(master, wide, tall):
    wide[0:OWN, 0:COLS] = master[:, 0, :]
    tall[0:OWN] = wide[0:OWN, 0:LANE]
    stripes = tall[...].T
    lane = lane_iota(STRIPE)
    acc = jnp.where(lane >= 4 * OWN, roll(wide[:, LANE:], 4 * OWN), 0.0)
    for q in range(4):
        acc = put(acc, lambda k: stripes[q * STRIPE : (q + 1) * STRIPE], 0, q * OWN, OWN)
    return acc


def z_body(place_at, parts, mine, other, grad, copies, wide, tall):
    wide[...] = jnp.zeros(wide.shape, f32)
    tall[...] = jnp.zeros(tall.shape, f32)
    masters = packed(mine, wide, tall), packed(other, wide, tall)
    for p in range(2):
        total = [parts[2 * k + p].astype(f32) for k in range(8)]
        while len(total) > 1:
            total = [a + b for a, b in zip(total[::2], total[1::2])]
        own = place_at[0] // 2 == p
        new = (jnp.where(own, *masters) - 0.1 * total[0]).astype(bf16)
        for d in range(16):
            copies[2 * d + p] = new

        @pl.when(own)
        def _():
            for q in range(4):
                tall[q * STRIPE : (q + 1) * STRIPE] = roll(total[0], -q * OWN)
            grad[:, 0, 0:LANE] = tall[...].T[:OWN]
            grad[:, 0, LANE:COLS] = roll(total[0], -4 * OWN)[:OWN, : COLS - LANE]


def z_sum(place_at, parts, mine, other):
    return pl.pallas_call(
        z_body,
        out_shape=(
            pltpu.VMEM((OWN, 1, COLS), f32),
            pltpu.VMEM((32, STRIPE, LANE), bf16),
        ),
        in_specs=[pl.BlockSpec(memory_space=pltpu.SMEM), IN_VMEM, IN_VMEM, IN_VMEM],
        out_specs=(IN_VMEM, IN_VMEM),
        scratch_shapes=[pltpu.VMEM((STRIPE, 2 * LANE), f32), pltpu.VMEM((LANE, LANE), f32)],
        name="z_sum",
    )(place_at, in_vmem(parts), in_vmem(mine), in_vmem(other))


def rows_body(parts, out, wide, rest):
    for d in range(32):
        x, half, quad = d // 8, d % 8 // 4, d % 4
        piece = parts[(x * 4 + quad) * 2 + half].astype(f32)
        wide[d] = piece
        rest[d * OWN : (d + 1) * OWN, :] = roll(piece, -4 * OWN)[:OWN]
    for t in range(ROWS // LANE):
        at = slice(t * LANE, (t + 1) * LANE)
        for q in range(4):
            acc = jnp.zeros((STRIPE, LANE), f32)
            for d in range(32):
                lo = max(d * OWN, t * LANE)
                hi = min((d + 1) * OWN, (t + 1) * LANE)
                if lo < hi:
                    acc = put(acc, lambda k: wide[d], q * OWN + lo - d * OWN, lo - t * LANE, hi - lo)
            out[q * STRIPE : (q + 1) * STRIPE, at] = acc.astype(bf16)
        out[4 * STRIPE :, at] = rest[at, :].T[:REST].astype(bf16)


def row_block(parts):
    return pl.pallas_call(
        rows_body,
        out_shape=pltpu.VMEM((COLS, ROWS), bf16),
        in_specs=[IN_VMEM],
        out_specs=IN_VMEM,
        scratch_shapes=[
            pltpu.VMEM((32, STRIPE, LANE), f32),
            pltpu.VMEM((ROWS, LANE), f32),
        ],
        name="row_block",
    )(in_vmem(parts))


def in_vmem(array):
    return pltpu.with_memory_space_constraint(array, pltpu.VMEM)


def in_hbm(array):
    return pltpu.with_memory_space_constraint(array, pltpu.HBM)


def exchange(array, axis):
    return lax.all_to_all(array, axis, split_axis=0, concat_axis=0, tiled=True)


def shards(hidden, cotangent, rewards, groups, lengths, master):
    swap = [(0, 1), (1, 0)]
    cot = cotangent.T
    core, x, half = (lax.axis_index(name).astype(jnp.int32) for name in (CORE, X, ZA))
    place_at = half * 2 + core
    base = (x * 2 + place_at % 2) * INFO
    mine = jnp.concatenate([rewards, groups, lengths])
    info = lax.dynamic_update_slice(jnp.zeros(LANE, jnp.int32), mine, (base,))
    info = lax.psum(info, (X, CORE))
    copies = jnp.broadcast_to(info, (32, LANE))
    copies, later_hidden, later_cot, info = lax.optimization_barrier((copies, hidden, cot, info))
    other_hidden = lax.ppermute(later_hidden, CORE, swap)
    other_cot = lax.ppermute(later_cot, CORE, swap)
    seen = exchange(copies, (ZH, ZA, ZB))
    parts = grad_parts(place_at[None], x[None], info, seen, cot, other_cot, hidden, other_hidden)
    parts, later_master = lax.optimization_barrier((parts, master.transpose(1, 0, 2)))
    parts = exchange(parts, X)
    other_master = lax.ppermute(later_master, ZA, swap)
    parts, later_master, other_master = lax.optimization_barrier((parts, later_master, other_master))
    parts = quad_sum(exchange(x_sum(parts), ZB))
    grad, copies = z_sum(place_at[None], exchange(parts, (ZH, ZA)), later_master, other_master)
    block = row_block(exchange(copies, (X, ZB)))
    block, grad = lax.optimization_barrier((block, grad))
    rollout = lax.all_gather(block.T[None], TP, axis=2, tiled=True)
    return (grad.transpose(1, 0, 2), rollout)


def solution(mesh):
    torus = Mesh(
        mesh.devices.reshape(4, 2, 4, 4, 2, mesh.shape["tp"]),
        (X, ZA, ZB, ZH, CORE, TP),
    )
    placed = (
        P(DP_FSDP, None),
        P(DP_FSDP, TP),
        P(DP_FSDP),
        P(DP_FSDP),
        P(DP_FSDP),
        P(FSDP, DP, TP),
    )
    return jax.shard_map(
        shards,
        mesh=torus,
        in_specs=placed,
        out_specs=(P(FSDP, DP, TP), P(FSDP, None, None)),
        check_vma=False,
    )
```

```python
import jax
import jax.numpy as jnp
from jax import lax
from jax.experimental import pallas as pl
from jax.experimental.pallas import tpu as pltpu
from jax.sharding import Mesh
from jax.sharding import PartitionSpec as P


GROUP = 16
X, ZA, ZB, ZH, CORE, TP = "x", "z_half", "z_quad", "z_hi", "core", "tp"
DP = (X, ZA, ZB)
FSDP = (ZH, CORE)
DP_FSDP = (X, ZA, ZB, ZH, CORE)

ROWS = 896
COLS = 144
OWN = 28
PART = 224
STRIPE = 32
REST = 16
LANE = 128
INFO = 12
IN_VMEM = pl.BlockSpec(memory_space=pltpu.VMEM)
f32 = jnp.float32
bf16 = jnp.bfloat16


def lane_iota(rows):
    return lax.broadcasted_iota(jnp.int32, (rows, LANE), 1)


def roll(tile, shift):
    shift = shift % LANE
    return tile if shift == 0 else pltpu.roll(tile, shift, 1)


def put(acc, tiles, src, dst, width):
    lane = lane_iota(acc.shape[0])
    done = 0
    while done < width:
        tile, off = divmod(src + done, LANE)
        take = min(LANE - off, width - done)
        at = dst + done
        moved = roll(tiles(tile), at - off)
        acc = jnp.where((lane >= at) & (lane < at + take), moved, acc)
        done += take
    return acc


def grad_body(place_at, x_at, info, seen, own_c, oth_c, own_h, oth_h, out, cot, wide, w_own, w_oth, edge, ready, sems, out_sems):
    def column(j):
        return pl.ds(pl.multiple_of((2 * j + place_at[0] % 2) * ROWS, LANE), ROWS)

    copies = [pltpu.make_async_copy(own_c, cot, sems.at[4])]
    copies += [pltpu.make_async_copy(own_h.at[:, column(j)], wide.at[j], sems.at[j]) for j in range(4)]
    for copy in copies:
        copy.start()

    lane = lane_iota(seen.shape[0])
    rewards = jnp.where((lane < 8 * INFO) & (lane % INFO < 4), seen[...], 0).astype(f32)
    labels = roll(seen[...], -4)
    row = lax.broadcasted_iota(jnp.int32, (8, LANE), 0)
    pos = lax.broadcasted_iota(jnp.int32, (8, LANE), 1)
    totals, squares = jnp.zeros((8, LANE), f32), jnp.zeros((8, LANE), f32)
    reward, length = jnp.zeros((8, LANE), jnp.int32), jnp.ones((8, LANE), jnp.int32)
    for s in range(8):
        core = place_at[0] % 2 if s < 4 else 1 - place_at[0] % 2
        base = (x_at[0] * 2 + core) * INFO + s % 4
        mates = jnp.where(labels == info[base + 4], rewards, 0.0)
        totals = jnp.where(row == s, jnp.sum(mates, axis=0, keepdims=True), totals)
        squares = jnp.where(row == s, jnp.sum(mates * mates, axis=0, keepdims=True), squares)
        reward = jnp.where(row == s, info[base], reward)
        length = jnp.where(row == s, info[base + 8], length)
    mean = jnp.sum(totals, axis=1, keepdims=True) / GROUP
    var = jnp.sum(squares, axis=1, keepdims=True) / GROUP - mean * mean
    adv = (reward.astype(f32) - mean) / jnp.sqrt(var + 1.0)
    scale = adv * jnp.where(pos < length, 1.0, 0.0) / length.astype(f32)
    copies[0].wait()
    for s in range(8):
        src, dst = (cot, w_own) if s < 4 else (oth_c, w_oth)
        at = (s % 4) * LANE
        dst[:, at : at + LANE] = (src[:, at : at + LANE].astype(f32) * scale[s : s + 1]).astype(bf16)

    def place(j, block):
        lo, hi = j * PART, (j + 1) * PART
        tiles = lambda k: block[:, k * LANE : (k + 1) * LANE]
        for x in range(4):
            for t in range(lo // LANE, -(-hi // LANE)):
                begin, end = max(lo, t * LANE), min(hi, (t + 1) * LANE)
                acc = edge[x] if t * LANE < lo else jnp.zeros((COLS, LANE), f32)
                acc = put(acc, tiles, x * PART + begin - lo, begin - t * LANE, end - begin)
                if end == (t + 1) * LANE:
                    ready[x, :, t * LANE : end] = acc.astype(bf16)
                else:
                    edge[x] = acc

    for j in range(4):
        other = jnp.dot(w_oth[...], oth_h[:, column(j)], preferred_element_type=f32)
        copies[1 + j].wait()
        place(j, jnp.dot(w_own[...], wide[j], preferred_element_type=f32) + other)
        tiles = slice(j * PART // LANE * LANE, (j + 1) * PART // LANE * LANE)
        copy = pltpu.make_async_copy(ready.at[:, :, tiles], out.at[:, :, tiles], out_sems.at[j])
        copy.start()
        copies.append(copy)
    for copy in copies[5:]:
        copy.wait()


def grad_parts(place_at, x_at, info, seen, own_c, oth_c, own_h, oth_h):
    tokens = own_h.shape[0]
    scalars = pl.BlockSpec(memory_space=pltpu.SMEM)
    in_place = pl.BlockSpec(memory_space=pl.ANY)
    return pl.pallas_call(
        grad_body,
        out_shape=jax.ShapeDtypeStruct((4, COLS, ROWS), bf16),
        in_specs=[scalars, scalars, scalars, IN_VMEM, in_place, IN_VMEM, in_place, IN_VMEM],
        out_specs=in_place,
        scratch_shapes=[
            pltpu.VMEM((COLS, tokens), bf16),
            pltpu.VMEM((4, tokens, ROWS), bf16),
            pltpu.VMEM((COLS, tokens), bf16),
            pltpu.VMEM((COLS, tokens), bf16),
            pltpu.VMEM((4, COLS, LANE), f32),
            pltpu.VMEM((4, COLS, ROWS), bf16),
            pltpu.SemaphoreType.DMA((5,)),
            pltpu.SemaphoreType.DMA((4,)),
        ],
        compiler_params=pltpu.CompilerParams(vmem_limit_bytes=24 << 20),
        name="grad_parts",
    )(place_at, x_at, info, in_vmem(seen), in_hbm(own_c), in_vmem(oth_c), in_hbm(own_h), in_vmem(oth_h))


def x_body(parts, out, total, rest):
    for t in range(ROWS // LANE):
        at = slice(t * LANE, (t + 1) * LANE)
        tile = (parts[0, :, at].astype(f32) + parts[1, :, at].astype(f32)) + (
            parts[2, :, at].astype(f32) + parts[3, :, at].astype(f32)
        )
        total[t] = tile
        rest[at, 0:REST] = tile[4 * STRIPE :, :].T
    rest[ROWS:, 0:REST] = jnp.zeros((8, REST), f32)
    lane = lane_iota(STRIPE)
    for j in range(4):
        for z in range(8):
            at = j * PART + z * OWN
            last = roll(rest[at : at + STRIPE], 4 * OWN)
            acc = jnp.where(lane >= 4 * OWN, last, 0.0)
            for q in range(4):
                acc = put(acc, lambda k: total[k, q * STRIPE : (q + 1) * STRIPE], at, q * OWN, OWN)
            half, quad = divmod(z, 4)
            out[quad * 8 + j * 2 + half] = acc.astype(bf16)


def x_sum(parts):
    return pl.pallas_call(
        x_body,
        out_shape=pltpu.VMEM((32, STRIPE, LANE), bf16),
        in_specs=[IN_VMEM],
        out_specs=IN_VMEM,
        scratch_shapes=[
            pltpu.VMEM((ROWS // LANE, COLS, LANE), f32),
            pltpu.VMEM((ROWS + 8, LANE), f32),
        ],
        name="x_sum",
    )(in_vmem(parts))


def quad_body(parts, out):
    for p in range(8):
        total = (parts[p].astype(f32) + parts[8 + p].astype(f32)) + (
            parts[16 + p].astype(f32) + parts[24 + p].astype(f32)
        )
        j, half = divmod(p, 2)
        for to in range(2):
            out[j * 4 + to * 2 + half] = total.astype(bf16)


def quad_sum(parts):
    return pl.pallas_call(
        quad_body,
        out_shape=pltpu.VMEM((16, STRIPE, LANE), bf16),
        in_specs=[IN_VMEM],
        out_specs=IN_VMEM,
        name="quad_sum",
    )(in_vmem(parts))


def packed(master, wide, tall):
    wide[0:OWN, 0:COLS] = master[:, 0, :]
    tall[0:OWN] = wide[0:OWN, 0:LANE]
    stripes = tall[...].T
    lane = lane_iota(STRIPE)
    acc = jnp.where(lane >= 4 * OWN, roll(wide[:, LANE:], 4 * OWN), 0.0)
    for q in range(4):
        acc = put(acc, lambda k: stripes[q * STRIPE : (q + 1) * STRIPE], 0, q * OWN, OWN)
    return acc


def z_body(place_at, parts, mine, other, grad, copies, wide, tall):
    wide[...] = jnp.zeros(wide.shape, f32)
    tall[...] = jnp.zeros(tall.shape, f32)
    masters = packed(mine, wide, tall), packed(other, wide, tall)
    for p in range(2):
        total = [parts[2 * k + p].astype(f32) for k in range(8)]
        while len(total) > 1:
            total = [a + b for a, b in zip(total[::2], total[1::2])]
        own = place_at[0] // 2 == p
        new = (jnp.where(own, *masters) - 0.1 * total[0]).astype(bf16)
        for d in range(16):
            copies[2 * d + p] = new

        @pl.when(own)
        def _():
            for q in range(4):
                tall[q * STRIPE : (q + 1) * STRIPE] = roll(total[0], -q * OWN)
            grad[:, 0, 0:LANE] = tall[...].T[:OWN]
            grad[:, 0, LANE:COLS] = roll(total[0], -4 * OWN)[:OWN, : COLS - LANE]


def z_sum(place_at, parts, mine, other):
    return pl.pallas_call(
        z_body,
        out_shape=(
            pltpu.VMEM((OWN, 1, COLS), f32),
            pltpu.VMEM((32, STRIPE, LANE), bf16),
        ),
        in_specs=[pl.BlockSpec(memory_space=pltpu.SMEM), IN_VMEM, IN_VMEM, IN_VMEM],
        out_specs=(IN_VMEM, IN_VMEM),
        scratch_shapes=[pltpu.VMEM((STRIPE, 2 * LANE), f32), pltpu.VMEM((LANE, LANE), f32)],
        name="z_sum",
    )(place_at, in_vmem(parts), in_vmem(mine), in_vmem(other))


def rows_body(parts, grad, out, grad_out, wide, rest, sem):
    copy = pltpu.make_async_copy(grad, grad_out, sem)
    copy.start()
    for d in range(32):
        x, half, quad = d // 8, d % 8 // 4, d % 4
        piece = parts[(x * 4 + quad) * 2 + half].astype(f32)
        wide[d] = piece
        rest[d * OWN : (d + 1) * OWN, :] = roll(piece, -4 * OWN)[:OWN]
    for t in range(ROWS // LANE):
        at = slice(t * LANE, (t + 1) * LANE)
        for q in range(4):
            acc = jnp.zeros((STRIPE, LANE), f32)
            for d in range(32):
                lo = max(d * OWN, t * LANE)
                hi = min((d + 1) * OWN, (t + 1) * LANE)
                if lo < hi:
                    acc = put(acc, lambda k: wide[d], q * OWN + lo - d * OWN, lo - t * LANE, hi - lo)
            out[q * STRIPE : (q + 1) * STRIPE, at] = acc.astype(bf16)
        out[4 * STRIPE :, at] = rest[at, :].T[:REST].astype(bf16)
    copy.wait()


def row_block(parts, grad):
    return pl.pallas_call(
        rows_body,
        out_shape=(pltpu.VMEM((COLS, ROWS), bf16), jax.ShapeDtypeStruct(grad.shape, f32)),
        in_specs=[IN_VMEM, IN_VMEM],
        out_specs=(IN_VMEM, pl.BlockSpec(memory_space=pl.ANY)),
        scratch_shapes=[
            pltpu.VMEM((32, STRIPE, LANE), f32),
            pltpu.VMEM((ROWS, LANE), f32),
            pltpu.SemaphoreType.DMA,
        ],
        name="row_block",
    )(in_vmem(parts), in_vmem(grad))


def in_vmem(array):
    return pltpu.with_memory_space_constraint(array, pltpu.VMEM)


def in_hbm(array):
    return pltpu.with_memory_space_constraint(array, pltpu.HBM)


def exchange(array, axis):
    return lax.all_to_all(array, axis, split_axis=0, concat_axis=0, tiled=True)


def shards(hidden, cotangent, rewards, groups, lengths, master):
    swap = [(0, 1), (1, 0)]
    cot = cotangent.T
    core, x, half = (lax.axis_index(name).astype(jnp.int32) for name in (CORE, X, ZA))
    place_at = half * 2 + core
    base = (x * 2 + place_at % 2) * INFO
    mine = jnp.concatenate([rewards, groups, lengths])
    info = lax.dynamic_update_slice(jnp.zeros(LANE, jnp.int32), mine, (base,))
    info = lax.psum(info, (X, CORE))
    copies = jnp.broadcast_to(info, (32, LANE))
    copies, later_hidden, later_cot, info = lax.optimization_barrier((copies, hidden, cot, info))
    other_hidden = lax.ppermute(later_hidden, CORE, swap)
    other_cot = lax.ppermute(later_cot, CORE, swap)
    seen = exchange(copies, (ZH, ZA, ZB))
    parts = grad_parts(place_at[None], x[None], info, seen, cot, other_cot, hidden, other_hidden)
    parts, later_master = lax.optimization_barrier((parts, master.transpose(1, 0, 2)))
    parts = exchange(parts, X)
    other_master = lax.ppermute(later_master, ZA, swap)
    parts, later_master, other_master = lax.optimization_barrier((parts, later_master, other_master))
    parts = quad_sum(exchange(x_sum(parts), ZB))
    grad, copies = z_sum(place_at[None], exchange(parts, (ZH, ZA)), later_master, other_master)
    block, grad = row_block(exchange(copies, (X, ZB)), grad)
    rollout = lax.all_gather(block, TP, axis=0, tiled=True)
    return (grad.transpose(1, 0, 2), rollout.T[None])


def solution(mesh):
    torus = Mesh(
        mesh.devices.reshape(4, 2, 4, 4, 2, mesh.shape["tp"]),
        (X, ZA, ZB, ZH, CORE, TP),
    )
    placed = (
        P(DP_FSDP, None),
        P(DP_FSDP, TP),
        P(DP_FSDP),
        P(DP_FSDP),
        P(DP_FSDP),
        P(FSDP, DP, TP),
    )
    return jax.shard_map(
        shards,
        mesh=torus,
        in_specs=placed,
        out_specs=(P(FSDP, DP, TP), P(FSDP, None, None)),
        check_vma=False,
    )
```

```python
import jax
import jax.numpy as jnp
from jax import lax
from jax.experimental import pallas as pl
from jax.experimental.pallas import tpu as pltpu
from jax.sharding import Mesh
from jax.sharding import PartitionSpec as P


GROUP = 16
X, ZA, ZB, ZH, CORE, TP = "x", "z_half", "z_quad", "z_hi", "core", "tp"
DP = (X, ZA, ZB)
FSDP = (ZH, CORE)
DP_FSDP = (X, ZA, ZB, ZH, CORE)

ROWS = 896
COLS = 144
OWN = 28
PART = 224
STRIPE = 32
REST = 16
LANE = 128
INFO = 12
IN_VMEM = pl.BlockSpec(memory_space=pltpu.VMEM)
f32 = jnp.float32
bf16 = jnp.bfloat16


def lane_iota(rows):
    return lax.broadcasted_iota(jnp.int32, (rows, LANE), 1)


def roll(tile, shift):
    shift = shift % LANE
    return tile if shift == 0 else pltpu.roll(tile, shift, 1)


def put(acc, tiles, src, dst, width):
    lane = lane_iota(acc.shape[0])
    done = 0
    while done < width:
        tile, off = divmod(src + done, LANE)
        take = min(LANE - off, width - done)
        at = dst + done
        moved = roll(tiles(tile), at - off)
        acc = jnp.where((lane >= at) & (lane < at + take), moved, acc)
        done += take
    return acc


def grad_body(place_at, x_at, info, seen, own_c, oth_c, own_h, oth_h, out, cot, wide, w_own, w_oth, edge, ready, sems, out_sems):
    def column(j):
        return pl.ds(pl.multiple_of((2 * j + place_at[0] % 2) * ROWS, LANE), ROWS)

    copies = [pltpu.make_async_copy(own_c, cot, sems.at[4])]
    copies += [pltpu.make_async_copy(own_h.at[:, column(j)], wide.at[j], sems.at[j]) for j in range(4)]
    for copy in copies:
        copy.start()

    lane = lane_iota(seen.shape[0])
    rewards = jnp.where((lane < 8 * INFO) & (lane % INFO < 4), seen[...], 0).astype(f32)
    labels = roll(seen[...], -4)
    row = lax.broadcasted_iota(jnp.int32, (8, LANE), 0)
    pos = lax.broadcasted_iota(jnp.int32, (8, LANE), 1)
    totals, squares = jnp.zeros((8, LANE), f32), jnp.zeros((8, LANE), f32)
    reward, length = jnp.zeros((8, LANE), jnp.int32), jnp.ones((8, LANE), jnp.int32)
    for s in range(8):
        core = place_at[0] % 2 if s < 4 else 1 - place_at[0] % 2
        base = (x_at[0] * 2 + core) * INFO + s % 4
        mates = jnp.where(labels == info[base + 4], rewards, 0.0)
        totals = jnp.where(row == s, jnp.sum(mates, axis=0, keepdims=True), totals)
        squares = jnp.where(row == s, jnp.sum(mates * mates, axis=0, keepdims=True), squares)
        reward = jnp.where(row == s, info[base], reward)
        length = jnp.where(row == s, info[base + 8], length)
    mean = jnp.sum(totals, axis=1, keepdims=True) / GROUP
    var = jnp.sum(squares, axis=1, keepdims=True) / GROUP - mean * mean
    adv = (reward.astype(f32) - mean) / jnp.sqrt(var + 1.0)
    scale = adv * jnp.where(pos < length, 1.0, 0.0) / length.astype(f32)
    copies[0].wait()
    for s in range(8):
        src, dst = (cot, w_own) if s < 4 else (oth_c, w_oth)
        at = (s % 4) * LANE
        dst[:, at : at + LANE] = (src[:, at : at + LANE].astype(f32) * scale[s : s + 1]).astype(bf16)

    def place(j, block):
        lo, hi = j * PART, (j + 1) * PART
        tiles = lambda k: block[:, k * LANE : (k + 1) * LANE]
        for x in range(4):
            for t in range(lo // LANE, -(-hi // LANE)):
                begin, end = max(lo, t * LANE), min(hi, (t + 1) * LANE)
                acc = edge[x] if t * LANE < lo else jnp.zeros((COLS, LANE), f32)
                acc = put(acc, tiles, x * PART + begin - lo, begin - t * LANE, end - begin)
                if end == (t + 1) * LANE:
                    ready[x, :, t * LANE : end] = acc.astype(bf16)
                else:
                    edge[x] = acc

    for j in range(4):
        other = jnp.dot(w_oth[...], oth_h[:, column(j)], preferred_element_type=f32)
        copies[1 + j].wait()
        place(j, jnp.dot(w_own[...], wide[j], preferred_element_type=f32) + other)
        tiles = slice(j * PART // LANE * LANE, (j + 1) * PART // LANE * LANE)
        copy = pltpu.make_async_copy(ready.at[:, :, tiles], out.at[:, :, tiles], out_sems.at[j])
        copy.start()
        copies.append(copy)
    for copy in copies[5:]:
        copy.wait()


def grad_parts(place_at, x_at, info, seen, own_c, oth_c, own_h, oth_h):
    tokens = own_h.shape[0]
    scalars = pl.BlockSpec(memory_space=pltpu.SMEM)
    in_place = pl.BlockSpec(memory_space=pl.ANY)
    return pl.pallas_call(
        grad_body,
        out_shape=jax.ShapeDtypeStruct((4, COLS, ROWS), bf16),
        in_specs=[scalars, scalars, scalars, IN_VMEM, in_place, IN_VMEM, in_place, IN_VMEM],
        out_specs=in_place,
        scratch_shapes=[
            pltpu.VMEM((COLS, tokens), bf16),
            pltpu.VMEM((4, tokens, ROWS), bf16),
            pltpu.VMEM((COLS, tokens), bf16),
            pltpu.VMEM((COLS, tokens), bf16),
            pltpu.VMEM((4, COLS, LANE), f32),
            pltpu.VMEM((4, COLS, ROWS), bf16),
            pltpu.SemaphoreType.DMA((5,)),
            pltpu.SemaphoreType.DMA((4,)),
        ],
        compiler_params=pltpu.CompilerParams(vmem_limit_bytes=24 << 20),
        name="grad_parts",
    )(place_at, x_at, info, in_vmem(seen), in_hbm(own_c), in_vmem(oth_c), in_hbm(own_h), in_vmem(oth_h))


def x_body(parts, out, total, rest):
    for t in range(ROWS // LANE):
        at = slice(t * LANE, (t + 1) * LANE)
        tile = (parts[0, :, at].astype(f32) + parts[1, :, at].astype(f32)) + (
            parts[2, :, at].astype(f32) + parts[3, :, at].astype(f32)
        )
        total[t] = tile
        rest[at, 0:REST] = tile[4 * STRIPE :, :].T
    rest[ROWS:, 0:REST] = jnp.zeros((8, REST), f32)
    lane = lane_iota(STRIPE)
    for j in range(4):
        for z in range(8):
            at = j * PART + z * OWN
            last = roll(rest[at : at + STRIPE], 4 * OWN)
            acc = jnp.where(lane >= 4 * OWN, last, 0.0)
            for q in range(4):
                acc = put(acc, lambda k: total[k, q * STRIPE : (q + 1) * STRIPE], at, q * OWN, OWN)
            half, quad = divmod(z, 4)
            out[quad * 8 + j * 2 + half] = acc.astype(bf16)


def x_sum(parts):
    return pl.pallas_call(
        x_body,
        out_shape=pltpu.VMEM((32, STRIPE, LANE), bf16),
        in_specs=[IN_VMEM],
        out_specs=IN_VMEM,
        scratch_shapes=[
            pltpu.VMEM((ROWS // LANE, COLS, LANE), f32),
            pltpu.VMEM((ROWS + 8, LANE), f32),
        ],
        name="x_sum",
    )(in_vmem(parts))


def quad_body(parts, out):
    for p in range(8):
        total = (parts[p].astype(f32) + parts[8 + p].astype(f32)) + (
            parts[16 + p].astype(f32) + parts[24 + p].astype(f32)
        )
        j, half = divmod(p, 2)
        for to in range(2):
            out[to * 8 + j * 2 + half] = total.astype(bf16)


def quad_sum(parts):
    return pl.pallas_call(
        quad_body,
        out_shape=pltpu.VMEM((16, STRIPE, LANE), bf16),
        in_specs=[IN_VMEM],
        out_specs=IN_VMEM,
        name="quad_sum",
    )(in_vmem(parts))


def packed(master, wide, tall):
    wide[0:OWN, 0:COLS] = master[:, 0, :]
    tall[0:OWN] = wide[0:OWN, 0:LANE]
    stripes = tall[...].T
    lane = lane_iota(STRIPE)
    acc = jnp.where(lane >= 4 * OWN, roll(wide[:, LANE:], 4 * OWN), 0.0)
    for q in range(4):
        acc = put(acc, lambda k: stripes[q * STRIPE : (q + 1) * STRIPE], 0, q * OWN, OWN)
    return acc


def z_body(place_at, parts, mine, other, grad, copies, wide, tall):
    wide[...] = jnp.zeros(wide.shape, f32)
    tall[...] = jnp.zeros(tall.shape, f32)
    masters = packed(mine, wide, tall), packed(other, wide, tall)
    for p in range(2):
        total = [parts[2 * k + p].astype(f32) for k in range(8)]
        while len(total) > 1:
            total = [a + b for a, b in zip(total[::2], total[1::2])]
        own = place_at[0] // 2 == p
        new = (jnp.where(own, *masters) - 0.1 * total[0]).astype(bf16)
        for d in range(16):
            copies[2 * d + p] = new

        @pl.when(own)
        def _():
            for q in range(4):
                tall[q * STRIPE : (q + 1) * STRIPE] = roll(total[0], -q * OWN)
            grad[:, 0, 0:LANE] = tall[...].T[:OWN]
            grad[:, 0, LANE:COLS] = roll(total[0], -4 * OWN)[:OWN, : COLS - LANE]


def z_sum(place_at, parts, mine, other):
    return pl.pallas_call(
        z_body,
        out_shape=(
            pltpu.VMEM((OWN, 1, COLS), f32),
            pltpu.VMEM((32, STRIPE, LANE), bf16),
        ),
        in_specs=[pl.BlockSpec(memory_space=pltpu.SMEM), IN_VMEM, IN_VMEM, IN_VMEM],
        out_specs=(IN_VMEM, IN_VMEM),
        scratch_shapes=[pltpu.VMEM((STRIPE, 2 * LANE), f32), pltpu.VMEM((LANE, LANE), f32)],
        name="z_sum",
    )(place_at, in_vmem(parts), in_vmem(mine), in_vmem(other))


def rows_body(parts, grad, out, grad_out, wide, rest, sem):
    copy = pltpu.make_async_copy(grad, grad_out, sem)
    copy.start()
    for d in range(32):
        x, half, quad = d // 8, d % 8 // 4, d % 4
        piece = parts[(x * 4 + quad) * 2 + half].astype(f32)
        wide[d] = piece
        rest[d * OWN : (d + 1) * OWN, :] = roll(piece, -4 * OWN)[:OWN]
    for t in range(ROWS // LANE):
        at = slice(t * LANE, (t + 1) * LANE)
        for q in range(4):
            acc = jnp.zeros((STRIPE, LANE), f32)
            for d in range(32):
                lo = max(d * OWN, t * LANE)
                hi = min((d + 1) * OWN, (t + 1) * LANE)
                if lo < hi:
                    acc = put(acc, lambda k: wide[d], q * OWN + lo - d * OWN, lo - t * LANE, hi - lo)
            out[q * STRIPE : (q + 1) * STRIPE, at] = acc.astype(bf16)
        out[4 * STRIPE :, at] = rest[at, :].T[:REST].astype(bf16)
    copy.wait()


def row_block(parts, grad):
    return pl.pallas_call(
        rows_body,
        out_shape=(pltpu.VMEM((COLS, ROWS), bf16), jax.ShapeDtypeStruct(grad.shape, f32)),
        in_specs=[IN_VMEM, IN_VMEM],
        out_specs=(IN_VMEM, pl.BlockSpec(memory_space=pl.ANY)),
        scratch_shapes=[
            pltpu.VMEM((32, STRIPE, LANE), f32),
            pltpu.VMEM((ROWS, LANE), f32),
            pltpu.SemaphoreType.DMA,
        ],
        name="row_block",
    )(in_vmem(parts), in_vmem(grad))


def in_vmem(array):
    return pltpu.with_memory_space_constraint(array, pltpu.VMEM)


def in_hbm(array):
    return pltpu.with_memory_space_constraint(array, pltpu.HBM)


def exchange(array, axis):
    return lax.all_to_all(array, axis, split_axis=0, concat_axis=0, tiled=True)


def shards(hidden, cotangent, rewards, groups, lengths, master):
    swap = [(0, 1), (1, 0)]
    cot = cotangent.T
    core, x, half = (lax.axis_index(name).astype(jnp.int32) for name in (CORE, X, ZA))
    place_at = half * 2 + core
    base = (x * 2 + place_at % 2) * INFO
    mine = jnp.concatenate([rewards, groups, lengths])
    info = lax.dynamic_update_slice(jnp.zeros(LANE, jnp.int32), mine, (base,))
    info = lax.psum(info, (X, CORE))
    copies = jnp.broadcast_to(info, (32, LANE))
    copies, later_hidden, later_cot, info = lax.optimization_barrier((copies, hidden, cot, info))
    other_hidden = lax.ppermute(later_hidden, CORE, swap)
    other_cot = lax.ppermute(later_cot, CORE, swap)
    seen = exchange(copies, (ZB, ZA, ZH))
    parts = grad_parts(place_at[None], x[None], info, seen, cot, other_cot, hidden, other_hidden)
    parts, later_master = lax.optimization_barrier((parts, master.transpose(1, 0, 2)))
    parts = exchange(parts, X)
    other_master = lax.ppermute(later_master, ZA, swap)
    parts, later_master, other_master = lax.optimization_barrier((parts, later_master, other_master))
    parts = quad_sum(exchange(x_sum(parts), ZB))
    grad, copies = z_sum(place_at[None], exchange(parts, (ZA, ZH)), later_master, other_master)
    block, grad = row_block(exchange(copies, (X, ZB)), grad)
    rollout = lax.all_gather(block, TP, axis=0, tiled=True)
    return (grad.transpose(1, 0, 2), rollout.T[None])


def solution(mesh):
    torus = Mesh(
        mesh.devices.reshape(4, 2, 4, 4, 2, mesh.shape["tp"]),
        (X, ZA, ZB, ZH, CORE, TP),
    )
    placed = (
        P(DP_FSDP, None),
        P(DP_FSDP, TP),
        P(DP_FSDP),
        P(DP_FSDP),
        P(DP_FSDP),
        P(FSDP, DP, TP),
    )
    return jax.shard_map(
        shards,
        mesh=torus,
        in_specs=placed,
        out_specs=(P(FSDP, DP, TP), P(FSDP, None, None)),
        check_vma=False,
    )
```
